32 devices in a mesh: dp: 8 (over z, y), mp: 4 (over x, core).
Axes of the slice: x: 2, y: 2, z: 4, core: 2. Of those that a mesh axis runs over, the one named last changes fastest.
Arguments:
- features: bfloat16 [3, 512, 16384], P(None, 'mp', 'dp'), may hold values from -6 to 6
- weights: bfloat16 [11, 512, 512], P(None, 'mp'), may hold values from -0.25 to 0.25
- sample_owner: int32 [3, 16384, 1], P(None, 'dp'), may hold values from 0 to 7; in each aligned block of 2048 rows (0 to 2047, 2048 to 4095, ..., all dimensions but the last counted through in order) at most 512 rows name the same one
- sample_row: int32 [3, 16384], P(None, 'dp'), may hold values from 0 to 2047
- edge_src: int32 [8, 16384], P(None, 'dp'), may hold values from 0 to 2047
- edge_dst: int32 [8, 16384], P(None, 'dp'), may hold values from 0 to 127
- edge_count: int32 [8, 8], P(None, 'dp'), may hold values from 128 to 2048
Outputs:
- updated: bfloat16 [3, 512, 1024], P(None, 'mp', 'dp')
The draws below stay inside these ranges and needn't reach their ends.
Inputs may be any that keep to these rules, and one draw needn't show every extreme that they name: `sample_owner`: among the 2048 entries of one node type in one block no owner appears more than 512 times; some owner appears exactly 512 times in some blocks.
All inputs are finite; a program needn't handle non-finite values.
Results may differ from the reference program's by a relative error of at most 0.0064.
Values may be sent and summed in bfloat16 or wider, within the bound.
No kernel may reach another device: no remote copies, remote signals or barrier semaphores. Data moves between devices by JAX's collectives and lax.ppermute only.
A program may use at most 64 MiB of HBM per device.

```python
import math
import jax
import jax.numpy as jnp
import numpy as np
from jax import lax

D = 512
RELS = 8
TYPES = 3
MATS = 11
ROWS_DEV = 2048
SAMP = 2048
SEEDS = 128
EDGES = 2048
CAP = 512
TABLE_ROWS = 16384
SAMPLES = 16384
EDGES_ALL = 16384
N_DP = 8


def plant(values, stream_key, smallest, high):
    extent = values.shape
    spot = [jax.random.randint(jax.random.fold_in(stream_key, axis), (), 0, extent[axis]) for axis in range(len(extent))]
    values = values.at[tuple(spot)].set(smallest)
    longest = extent.index(max(extent))
    spot[longest] = (spot[longest] + 1) % extent[longest]
    return values.at[tuple(spot)].set(high)


def level_of(rng, shape, cuts, low, largest):
    loudness = 1.0
    for position, shards_of in cuts:
        draws = jax.random.uniform(jax.random.fold_in(jax.random.fold_in(rng, 6), position), (shards_of,), jnp.float32, low / len(cuts), largest / len(cuts))
        loudness = loudness * jnp.repeat(jnp.exp(draws), shape[position] // shards_of).reshape((-1,) + (1,) * (len(shape) - 1 - position))
    return loudness


def assign_block(own_key, own, number, rows, count, top, limit, lean):
    sequence = jax.random.permutation(own_key, count)
    heavy_load, common = portions_of(count, rows * top, limit, lean, True), portions_of(count, rows * top, limit, lean, False)
    places = jnp.arange(count)

    def named(tallies, rotation):
        used = int((tallies > 0).sum())
        fixed = max(1, used // 4)
        passed = fixed + (places - fixed + rotation * (used - fixed)) % max(1, count - fixed)
        return jnp.zeros((count,), jnp.int32).at[sequence[jnp.where(places < fixed, places, passed)]].set(jnp.asarray(tallies, jnp.int32))

    tallies = jnp.where(number % 4 == 0, named(heavy_load, number // 4), named(common, number - number // 4 - 1))
    mixed = jax.random.permutation(jax.random.fold_in(own, 3), count)
    source_of, sink = mixed[0:count // 2 * 2:2], mixed[1:count // 2 * 2:2]
    margin = jnp.minimum(tallies[source_of] - 1, limit - tallies[sink]) // 2
    margin = jnp.where((source_of == sequence[0]) | (sink == sequence[0]) | (tallies[sink] == 0), 0, jnp.maximum(margin, 0))
    passed = jax.random.randint(jax.random.fold_in(own, 4), (count // 2,), 0, 1 << 20) % (margin + 1)
    tallies = tallies.at[source_of].add(-passed).at[sink].add(passed)
    labels = jnp.searchsorted(jnp.cumsum(tallies), jnp.arange(rows * top), side="right").astype(jnp.int32)
    listing = labels.reshape(top, rows).T
    listing = listing[jax.random.permutation(jax.random.fold_in(own, 1), rows)]
    rotation = jax.random.randint(jax.random.fold_in(own, 2), (rows, 1), 0, top)
    return jnp.take_along_axis(listing, (jnp.arange(top)[None, :] + rotation) % top, axis=1)


def portions_of(count, total, limit, skew, full):
    loads = [(1 << 20) // math.isqrt(standing ** skew) + 1 for standing in range(1, count + 1)]
    largest = limit if full else min(limit, max(-(-total // count), total * loads[0] // sum(loads)))
    least = 1 if total - largest >= count - 1 else 0
    given, rest = [largest] + [least] * (count - 1), total - largest - least * (count - 1)
    while rest > 0:
        free = [i for i in range(1, count) if given[i] < largest] or [i for i in range(1, count) if given[i] < limit]
        whole, left = sum([loads[i] for i in free]), rest
        for i in free:
            more = min(limit - given[i], max(1, left * loads[i] // whole), rest)
            given[i] = given[i] + more
            rest = rest - more
    return np.array(given)


def normal_values(key, dims, width, most, split=(), kind=jnp.bfloat16):
    drawn = jax.random.normal(key, dims, jnp.float32) * width
    if len(split) > 0:
        drawn = level_of(key, dims, split, -0.22, 0.18) * drawn
    return jnp.clip(drawn, min=-most, max=most).astype(kind)


def setup_inputs(seed: int = 0) -> dict:
    arg_keys = jax.random.split(jax.random.key(seed), 8)
    features = normal_values(arg_keys[0], (TYPES, D, TABLE_ROWS), 1.0, 6.0, ((1, 4), (2, 8)))
    weights = normal_values(arg_keys[1], (MATS, D, D), D ** -0.5, 0.25, ((1, 4),))
    sample_owner_keys = jax.random.split(jax.random.fold_in(arg_keys[2], 1), TYPES * SAMPLES // SAMP)
    sample_owner_turns = jax.random.permutation(jax.random.fold_in(arg_keys[2], 3), TYPES * SAMPLES // SAMP)
    sample_owner = jax.vmap(lambda own, number: assign_block(jax.random.fold_in(arg_keys[2], 2), own, number, SAMP, N_DP, 1, CAP, 2))(sample_owner_keys, sample_owner_turns).reshape((TYPES, SAMPLES, 1))
    sample_row = plant(jax.random.randint(arg_keys[3], (TYPES, SAMPLES), 0, ROWS_DEV), jax.random.fold_in(arg_keys[3], 1), 0, ROWS_DEV - 1).astype(jnp.int32)
    edge_src = plant(jax.random.randint(arg_keys[4], (RELS, EDGES_ALL), 0, SAMP), jax.random.fold_in(arg_keys[4], 1), 0, SAMP - 1).astype(jnp.int32)
    edge_dst = plant(jax.random.randint(arg_keys[5], (RELS, EDGES_ALL), 0, SEEDS), jax.random.fold_in(arg_keys[5], 1), 0, SEEDS - 1).astype(jnp.int32)
    edge_count = plant(jax.random.randint(arg_keys[6], (RELS, N_DP), EDGES // 16, EDGES + 1), jax.random.fold_in(arg_keys[6], 1), EDGES // 16, EDGES).astype(jnp.int32)
    return {"features": features, "weights": weights, "sample_owner": sample_owner, "sample_row": sample_row, "edge_src": edge_src, "edge_dst": edge_dst, "edge_count": edge_count}


RELATION_SOURCE = (0, 1, 0, 1, 2, 0, 2, 1)
RELATION_TARGET = (1, 0, 0, 2, 1, 2, 0, 1)


def reference(features, weights, sample_owner, sample_row, edge_src, edge_dst, edge_count):
    row_index = (sample_owner[:, :, 0] * ROWS_DEV + sample_row).astype(jnp.int32)
    block_index = row_index.reshape(TYPES, N_DP, SAMP).transpose(1, 0, 2)
    block_src = edge_src.reshape(RELS, N_DP, EDGES).transpose(1, 0, 2)
    block_dst = edge_dst.reshape(RELS, N_DP, EDGES).transpose(1, 0, 2)
    block_count = edge_count.transpose(1, 0)

    def one_block(inputs):
        index_here, src_here, dst_here, count_here = inputs
        fetched = [jnp.take(features[node_kind], index_here[node_kind], axis=1).T for node_kind in range(TYPES)]
        typed = [jnp.dot(fetched[node_kind][:SEEDS], weights[RELS + node_kind], preferred_element_type=jnp.float32) for node_kind in range(TYPES)]
        slot_ids = jnp.arange(EDGES, dtype=jnp.int32)
        for relation in range(RELS):
            live_edge = (slot_ids < count_here[relation]).astype(jnp.float32)
            sources = jnp.take(fetched[RELATION_SOURCE[relation]], src_here[relation], axis=0).astype(jnp.float32)
            summed = jax.ops.segment_sum(sources * live_edge[:, None], dst_here[relation], num_segments=SEEDS)
            degree = jax.ops.segment_sum(live_edge, dst_here[relation], num_segments=SEEDS)
            message = (summed / jnp.maximum(degree, 1.0)[:, None]).astype(jnp.bfloat16)
            target = RELATION_TARGET[relation]
            typed[target] = typed[target] + jnp.dot(message, weights[relation], preferred_element_type=jnp.float32)
        return jnp.stack([jax.nn.relu(value).astype(jnp.bfloat16) for value in typed])

    result = lax.map(one_block, (block_index, block_src, block_dst, block_count))
    return result.transpose(1, 3, 0, 2).reshape(TYPES, result.shape[3], N_DP * SEEDS)
```

```python
import functools

import jax
import jax.numpy as jnp
from jax import lax
from jax.experimental import pallas as pl
from jax.experimental.pallas import tpu as pltpu
from jax.sharding import PartitionSpec as P

SEEDS = 128
LANES = 128
SHIFT = 16
LOW = (1 << SHIFT) - 1

RELATION_SOURCE = (0, 1, 0, 1, 2, 0, 2, 1)
RELATION_TARGET = (1, 0, 0, 2, 1, 2, 0, 1)
AXES = ("dp", "mp")
NT = (((1,), (1,)), ((), ()))
NN = (((1,), (0,)), ((), ()))
VMEM_LIMIT = 56 * 1024 * 1024


def dot(left, right, dims=NN):
    return lax.dot_general(left, right, dims, preferred_element_type=jnp.float32)


def iota(shape, axis):
    return lax.broadcasted_iota(jnp.int32, shape, axis)


def as_bf16(mask):
    return jnp.where(mask, 1.0, 0.0).astype(jnp.bfloat16)


def prep_body(groups, capacity, count_ref, owner_ref, row_ref, src_ref, dst_ref, req_ref, edge_ref):
    kinds, chunks, _ = owner_ref.shape
    rels = src_ref.shape[0]
    stack = chunks * groups
    upper = as_bf16(iota((LANES, LANES), 0) <= iota((LANES, LANES), 1))
    ones = jnp.ones((LANES, LANES), jnp.bfloat16)
    line, other = iota((stack, stack), 0), iota((stack, stack), 1)
    earlier = as_bf16((other < line) & (line % groups == other % groups))
    owner_ids = iota((groups, LANES), 0)
    tables = []
    for kind in range(kinds):
        owner = owner_ref[kind]
        row = row_ref[kind]
        masks = [owner[c : c + 1] == owner_ids for c in range(chunks)]
        hot = jnp.concatenate([jnp.where(mask, 1.0, 0.0) for mask in masks], axis=0)
        hot16 = hot.astype(jnp.bfloat16)
        totals = dot(hot16, ones).astype(jnp.bfloat16)
        inclusive = dot(hot16, upper) + dot(earlier, totals)
        ranks = jnp.sum((hot * inclusive).reshape(chunks, groups, LANES), axis=1)
        rank = ranks.astype(jnp.int32) - 1
        tables.append(owner * capacity + rank)
        high, low = (row >> 7).astype(jnp.float32), (row & 127).astype(jnp.float32)
        left = jnp.concatenate(
            [
                jnp.concatenate(
                    [
                        jnp.where(masks[c], high[c : c + 1], 0.0),
                        jnp.where(masks[c], low[c : c + 1], 0.0),
                    ],
                    axis=0,
                )
                for c in range(chunks)
            ],
            axis=1,
        ).astype(jnp.bfloat16)
        rank_ids = iota((capacity, LANES), 0)
        right = jnp.concatenate(
            [as_bf16(rank[c : c + 1] == rank_ids) for c in range(chunks)], axis=1
        )
        picked = dot(left, right, NT)
        rows = picked[:groups] * 128.0 + picked[groups:]
        for group in range(groups):
            req_ref[group, kind : kind + 1, :] = rows[group : group + 1].astype(jnp.int32)
    edge_chunks = src_ref.shape[1]
    place = iota((edge_chunks, LANES), 0) * LANES + iota((edge_chunks, LANES), 1)
    target_ids = iota((SEEDS, LANES), 0)
    eight = jnp.ones((8, LANES), jnp.bfloat16)
    degrees = []
    for rel in range(rels):
        src, dst = src_ref[rel], dst_ref[rel]
        table = tables[RELATION_SOURCE[rel]]
        low, high = src & 127, src >> 7
        slot = jnp.zeros_like(src)
        for c in range(chunks):
            line = jnp.broadcast_to(table[c : c + 1], src.shape)
            found = jnp.take_along_axis(line, low, axis=1)
            slot = jnp.where(high == c, found, slot)
        live = place < count_ref[rel, 0]
        edge_ref[rel * edge_chunks : (rel + 1) * edge_chunks, :] = jnp.where(
            live, (slot << SHIFT) | dst, -1
        )
        target = jnp.where(live, dst, -1)
        tally = jnp.zeros((SEEDS, LANES), jnp.float32)
        for c in range(edge_chunks):
            tally = tally + jnp.where(target[c : c + 1] == target_ids, 1.0, 0.0)
        degrees.append(dot(eight, tally.astype(jnp.bfloat16), NT)[:1])
    base = rels * edge_chunks
    lane = iota((1, LANES), 1)
    seeds = [(table[:1] << SHIFT) | lane for table in tables]
    seeds = seeds + [jnp.full((1, LANES), -1, jnp.int32)] * (8 - kinds)
    edge_ref[base : base + 8, :] = jnp.concatenate(seeds, axis=0)
    edge_ref[base + 8 : base + 8 + rels, :] = jnp.concatenate(degrees, axis=0).astype(jnp.int32)


def pick_body(req_ref, own_ref, oth_ref, out_ref):
    capacity = req_ref.shape[3]
    table_rows = own_ref.shape[2]
    wide = jnp.broadcast_to(req_ref[0, 0], (8, capacity))
    column = jnp.transpose(wide)[:, :1]
    hot = as_bf16(column == iota((capacity, table_rows), 1))
    table = jnp.concatenate([own_ref[0], oth_ref[0]], axis=0)
    out_ref[0, 0] = dot(hot, table, NT).astype(jnp.bfloat16)


def relate_body(rels_here, kind, rels, me_ref, edge_ref, pick_ref, own_ref, oth_ref, out_ref, msg_ref):
    _, blocks, capacity, width = pick_ref.shape
    half = capacity // 2
    edge_chunks = (edge_ref.shape[1] - 8 - rels) // rels
    base = rels * edge_chunks
    first = me_ref[0] * capacity

    def counts(packed):
        slot = (packed >> SHIFT) - first
        mine = (slot >= 0) & (slot < capacity)
        upper = jnp.where(slot >= half, 1, 0)
        left = jnp.where(mine, slot - upper * half, -1)
        right = jnp.where(mine, (packed & LOW) + upper * SEEDS, -1)
        lines = packed.shape[0]
        left_ids, right_ids = iota((half, LANES), 0), iota((2 * SEEDS, LANES), 0)
        left_hot = jnp.concatenate(
            [as_bf16(left[c : c + 1] == left_ids) for c in range(lines)], axis=1
        )
        right_hot = jnp.concatenate(
            [as_bf16(right[c : c + 1] == right_ids) for c in range(lines)], axis=1
        )
        table = dot(right_hot, left_hot, NT).astype(jnp.bfloat16)
        return jnp.concatenate([table[:SEEDS], table[SEEDS:]], axis=1)

    def one_block(block, carry):
        degree = edge_ref[block, base + 8 : base + 8 + rels, :].astype(jnp.float32)
        inverse = jnp.transpose(1.0 / jnp.maximum(degree, 1.0))
        spot = pl.ds(pl.multiple_of(block * SEEDS, SEEDS), SEEDS)
        for order, rel in enumerate(rels_here):
            packed = edge_ref[block, rel * edge_chunks : (rel + 1) * edge_chunks, :]
            table = counts(packed)
            summed = dot(table, pick_ref[RELATION_SOURCE[rel], block])
            msg_ref[order, spot, :] = (summed * inverse[:, rel : rel + 1]).astype(jnp.bfloat16)
        packed = edge_ref[block, base + kind : base + kind + 1, :]
        table = counts(packed)
        msg_ref[len(rels_here), spot, :] = dot(table, pick_ref[kind, block]).astype(jnp.bfloat16)
        return carry

    lax.fori_loop(0, blocks, one_block, 0)
    total = None
    for order, matrix in enumerate(tuple(rels_here) + (rels + kind,)):
        weight = jnp.concatenate([own_ref[matrix], oth_ref[matrix]], axis=0)
        term = dot(msg_ref[order], weight)
        total = term if total is None else total + term
    pieces_x, _, _, _, lanes = out_ref.shape
    for piece in range(pieces_x):
        for block in range(blocks):
            for core in range(2):
                at = (piece * 2 + core) * lanes
                out_ref[piece, block, core] = total[
                    block * SEEDS : (block + 1) * SEEDS, at : at + lanes
                ].astype(jnp.bfloat16)


def final_body(part_refs, out_ref):
    kinds = out_ref.shape[0]
    for kind in range(kinds):
        total = part_refs[4 * kind][...].astype(jnp.float32)
        for order in range(1, 4):
            total = total + part_refs[4 * kind + order][...].astype(jnp.float32)
        out_ref[kind] = jnp.transpose(jnp.maximum(total, 0.0)).astype(jnp.bfloat16)


def params(**more):
    return pltpu.CompilerParams(vmem_limit_bytes=VMEM_LIMIT, **more)


def per_device(groups, cores, features, weights, sample_owner, sample_row, edge_src, edge_dst, edge_count):
    kinds, width, table_rows = features.shape
    sampled = sample_row.shape[1]
    capacity = 2 * sampled // groups
    rels, edges = edge_src.shape
    full = weights.shape[2]
    blocks = groups // 2
    pieces_x = cores // 2
    devices = [(dp, mp) for dp in range(groups) for mp in range(cores)]

    def send(value, target):
        pairs = []
        for dp, mp in devices:
            to_dp, to_mp = target(dp, mp)
            pairs.append((dp * cores + mp, to_dp * cores + to_mp))
        return lax.ppermute(value, AXES, pairs)

    def swap_core(dp, mp):
        return dp, mp ^ 1

    def spread(step):
        def target(dp, mp):
            bit, core = (dp >> 1) & 1, mp & 1
            return ((dp ^ step) & ~2) | (core << 1), (mp & ~1) | bit

        return target

    dp, mp = lax.axis_index("dp"), lax.axis_index("mp")
    core, bit = mp & 1, (dp >> 1) & 1
    steps = [step for step in range(groups) if step & 2 == 0]

    features_oth = send(features, swap_core)
    weights_oth = send(weights, swap_core)

    lines = kinds, sampled // LANES, LANES
    edge_lines = rels, edges // LANES, LANES
    edge_rows = rels * (edges // LANES) + 8 + rels
    smem = pl.BlockSpec(memory_space=pltpu.SMEM)
    vmem = pl.BlockSpec(memory_space=pltpu.VMEM)
    requests, packed = pl.pallas_call(
        functools.partial(prep_body, groups, capacity),
        out_shape=(
            jax.ShapeDtypeStruct((groups, kinds, capacity), jnp.int32),
            jax.ShapeDtypeStruct((edge_rows, LANES), jnp.int32),
        ),
        in_specs=[smem] + [vmem] * 4,
        out_specs=(vmem, vmem),
        compiler_params=params(),
        name="prep",
    )(
        edge_count,
        sample_owner.reshape(lines),
        sample_row.reshape(lines),
        edge_src.reshape(edge_lines),
        edge_dst.reshape(edge_lines),
    )
    asked, listed = [], []
    for step in steps:
        owner = ((dp ^ step) & ~2) | (core << 1)
        mine = lax.dynamic_index_in_dim(requests, owner, 0, keepdims=False)
        asked.append(send(mine, spread(step)))
    for step in steps:
        listed.append(send(packed, spread(step)))
    asked = jnp.stack(asked, axis=1).reshape(kinds, blocks, 1, capacity)
    listed = jnp.stack(listed)

    picked = pl.pallas_call(
        pick_body,
        out_shape=jax.ShapeDtypeStruct((kinds, blocks, capacity, 2 * width), jnp.bfloat16),
        grid=(kinds, blocks),
        in_specs=[
            pl.BlockSpec((1, 1, 1, capacity), lambda t, g: (t, g, 0, 0)),
            pl.BlockSpec((1, width, table_rows), lambda t, g: (t, 0, 0)),
            pl.BlockSpec((1, width, table_rows), lambda t, g: (t, 0, 0)),
        ],
        out_specs=pl.BlockSpec((1, 1, capacity, 2 * width), lambda t, g: (t, g, 0, 0)),
        compiler_params=params(),
        cost_estimate=pl.CostEstimate(
            flops=2 * kinds * blocks * capacity * table_rows * 2 * width,
            bytes_accessed=6 * 2**20,
            transcendentals=0,
        ),
        name="pick",
    )(asked, features, features_oth)

    me = dp.reshape(1)
    parts = []
    for kind in range(kinds):
        rels_here = tuple(r for r in range(rels) if RELATION_TARGET[r] == kind)
        typed = pl.pallas_call(
            functools.partial(relate_body, rels_here, kind, rels),
            out_shape=jax.ShapeDtypeStruct(
                (pieces_x, blocks, 2, SEEDS, full // cores), jnp.bfloat16
            ),
            in_specs=[smem] + [vmem] * 4,
            out_specs=vmem,
            scratch_shapes=[
                pltpu.VMEM((len(rels_here) + 1, blocks * SEEDS, 2 * width), jnp.bfloat16)
            ],
            compiler_params=params(),
            cost_estimate=pl.CostEstimate(
                flops=2 * len(rels_here) * blocks * edges * capacity * SEEDS,
                bytes_accessed=6 * 2**20,
                transcendentals=0,
            ),
            name=f"relate{kind}",
        )(me, listed, picked, weights, weights_oth)

        def merge(kept, sent, target):
            got = send(sent, target)
            return (kept.astype(jnp.float32) + got.astype(jnp.float32)).astype(jnp.bfloat16)

        size = pieces_x
        while size > 1:
            size //= 2
            up = ((mp >> 1) // size) & 1
            halves = typed.reshape((2, size) + typed.shape[1:])
            kept = lax.dynamic_index_in_dim(halves, up, 0, keepdims=False)
            sent = lax.dynamic_index_in_dim(halves, 1 - up, 0, keepdims=False)
            typed = merge(kept, sent, lambda d, m, size=size: (d, m ^ (2 * size)))
        typed = typed[0]
        left = list(steps)
        for flip in [1] + [1 << i for i in range(3, groups.bit_length() - 1)]:
            keep = [i for i, step in enumerate(left) if step & flip == 0]
            away = [i for i, step in enumerate(left) if step & flip]
            kept = jnp.stack([typed[i] for i in keep])
            sent = jnp.stack([typed[i] for i in away])
            typed = merge(kept, sent, lambda d, m, flip=flip: (d ^ flip, m))
            left = [left[i] for i in keep]
        for order, step in enumerate(left):
            for turn in range(2):
                value = lax.dynamic_index_in_dim(typed[order], bit ^ turn, 0, keepdims=False)

                def target(d, m, step=step, turn=turn):
                    return ((d ^ step) & ~2) | ((m & 1) << 1), (m & ~1) | (((d >> 1) & 1) ^ turn)

                parts.append(send(value, target))

    count = len(parts)
    return pl.pallas_call(
        lambda *refs: final_body(refs[:count], refs[count]),
        out_shape=jax.ShapeDtypeStruct((kinds, full // cores, SEEDS), jnp.bfloat16),
        in_specs=[vmem] * count,
        out_specs=vmem,
        compiler_params=params(),
        name="final",
    )(*parts)


def solution(mesh):
    return jax.shard_map(
        functools.partial(per_device, mesh.shape["dp"], mesh.shape["mp"]),
        mesh=mesh,
        in_specs=(
            P(None, "mp", "dp"),
            P(None, "mp", None),
            P(None, "dp", None),
            P(None, "dp"),
            P(None, "dp"),
            P(None, "dp"),
            P(None, "dp"),
        ),
        out_specs=P(None, "mp", "dp"),
        check_vma=False,
    )
```

```python
import functools

import jax
import jax.numpy as jnp
from jax import lax
from jax.experimental import pallas as pl
from jax.experimental.pallas import tpu as pltpu
from jax.sharding import PartitionSpec as P

SEEDS = 128
LANES = 128
SHIFT = 16
LOW = (1 << SHIFT) - 1

RELATION_SOURCE = (0, 1, 0, 1, 2, 0, 2, 1)
RELATION_TARGET = (1, 0, 0, 2, 1, 2, 0, 1)
AXES = ("dp", "mp")
NT = (((1,), (1,)), ((), ()))
NN = (((1,), (0,)), ((), ()))
VMEM_LIMIT = 56 * 1024 * 1024


def dot(left, right, dims=NN):
    return lax.dot_general(left, right, dims, preferred_element_type=jnp.float32)


def iota(shape, axis):
    return lax.broadcasted_iota(jnp.int32, shape, axis)


def as_bf16(mask):
    return jnp.where(mask, 1.0, 0.0).astype(jnp.bfloat16)


def tiled(row, lines):
    packed = jnp.broadcast_to(row, (16, LANES)).astype(jnp.bfloat16)
    return jnp.concatenate([packed] * (lines // 16), axis=0)


def one_zero(mask):
    one = jnp.ones(mask.shape, jnp.bfloat16)
    return jnp.where(mask, one, jnp.zeros_like(one))


def ids(shape, axis, start=0):
    return (iota(shape, axis) + start).astype(jnp.float32).astype(jnp.bfloat16)


def message_rows(rels, edge_chunks, kinds, capacity):
    seeds = rels * edge_chunks
    degrees = seeds + 8
    requests = degrees + 8
    return seeds, degrees, requests, requests + -(-kinds * capacity // LANES // 8) * 8


def prep_body(groups, capacity, steps, place_ref, count_ref, owner_ref, row_ref, src_ref, dst_ref, *refs):
    kinds, chunks, _ = owner_ref.shape
    out_refs, req_ref, hold_ref = refs[: len(steps)], refs[-2], refs[-1]
    rels, edges = src_ref.shape
    edge_chunks = edges // LANES
    seed_row, degree_row, request_row, _ = message_rows(rels, edge_chunks, kinds, capacity)
    parts = capacity // LANES
    stack = chunks * groups
    upper = as_bf16(iota((LANES, LANES), 0) <= iota((LANES, LANES), 1))
    ones = jnp.ones((LANES, LANES), jnp.bfloat16)
    line, other = iota((stack, stack), 0), iota((stack, stack), 1)
    earlier = as_bf16((other < line) & (line % groups == other % groups))
    owner_ids = iota((groups, LANES), 0)
    part_ids = iota((groups * parts, LANES), 0)
    lane_ids = ids((LANES, LANES), 0)
    tables = []
    for kind in range(kinds):
        owner = owner_ref[kind]
        row = jnp.concatenate(
            [row_ref[kind : kind + 1, c * LANES : (c + 1) * LANES] for c in range(chunks)], axis=0
        )
        hot = jnp.concatenate(
            [jnp.where(owner[c : c + 1] == owner_ids, 1.0, 0.0) for c in range(chunks)], axis=0
        )
        hot16 = hot.astype(jnp.bfloat16)
        totals = dot(hot16, ones).astype(jnp.bfloat16)
        inclusive = dot(hot16, upper) + dot(earlier, totals)
        ranks = jnp.sum((hot * inclusive).reshape(chunks, groups, LANES), axis=1)
        table = owner * capacity + ranks.astype(jnp.int32) - 1
        tables.append(table)
        part, low = table >> 7, (table & 127).astype(jnp.float32)
        high_digit, low_digit = (row >> 7).astype(jnp.float32), (row & 127).astype(jnp.float32)
        left = []
        for c in range(chunks):
            mask = part[c : c + 1] == part_ids
            left.append(
                jnp.concatenate(
                    [
                        jnp.where(mask, high_digit[c : c + 1], 0.0),
                        jnp.where(mask, low_digit[c : c + 1], 0.0),
                    ],
                    axis=0,
                )
            )
        left = jnp.concatenate(left, axis=1).astype(jnp.bfloat16)
        right = jnp.concatenate(
            [one_zero(tiled(low[c : c + 1], LANES) == lane_ids) for c in range(chunks)], axis=1
        )
        picked = dot(left, right, NT)
        rows = picked[: groups * parts] * 128.0 + picked[groups * parts :]
        rows = rows.astype(jnp.int32)
        for group in range(groups):
            req_ref[kind, group] = rows[group * parts : (group + 1) * parts]
    rel_ids = iota((rels, LANES), 0)
    wide = []
    for c in range(chunks):
        line = jnp.zeros((rels, LANES), jnp.int32)
        for kind in range(kinds):
            match = functools.reduce(
                lambda p, q: p | q, [rel_ids == r for r in range(rels) if RELATION_SOURCE[r] == kind]
            )
            line = jnp.where(match, tables[kind][c : c + 1], line)
        wide.append(line)
    limit = jnp.zeros((rels, LANES), jnp.int32)
    for rel in range(rels):
        limit = jnp.where(rel_ids == rel, count_ref[0, rel], limit)
    tallies = [jnp.zeros((SEEDS, LANES), jnp.bfloat16)] * rels
    target_ids = ids((SEEDS, LANES), 0)
    for e in range(edge_chunks):
        span = slice(e * LANES, (e + 1) * LANES)
        src, dst = src_ref[:, span], dst_ref[:, span]
        low, high = src & 127, src >> 7
        slot = jnp.zeros_like(src)
        for c in range(chunks):
            slot = jnp.where(high == c, jnp.take_along_axis(wide[c], low, axis=1), slot)
        live = iota((rels, LANES), 1) + e * LANES < limit
        hold_ref[e * rels : (e + 1) * rels, :] = jnp.where(live, (slot << SHIFT) | dst, -1)
        target = jnp.where(live, dst, -1).astype(jnp.float32)
        for rel in range(rels):
            tallies[rel] = tallies[rel] + one_zero(tiled(target[rel : rel + 1], SEEDS) == target_ids)
    eight = jnp.ones((8, LANES), jnp.bfloat16)
    degrees = [dot(eight, tally, NT)[:1] for tally in tallies]
    lane = iota((1, LANES), 1)
    seeds = [(table[:1] << SHIFT) | lane for table in tables]
    seeds = seeds + [jnp.full((1, LANES), -1, jnp.int32)] * (8 - kinds)
    hold_ref[seed_row : seed_row + 8, :] = jnp.concatenate(seeds, axis=0)
    hold_ref[degree_row : degree_row + rels, :] = jnp.concatenate(degrees, axis=0).astype(jnp.int32)
    for step, out_ref in zip(steps, out_refs):
        to = ((place_ref[0] ^ step) & ~2) | (place_ref[1] << 1)
        out_ref[:request_row, :] = hold_ref[:request_row, :]
        for kind in range(kinds):
            at = request_row + kind * parts
            out_ref[at : at + parts, :] = req_ref[kind, to]


def pick_body(blocks, request_row, *refs):
    msg_refs, own_ref, oth_ref, out_ref = refs[:blocks], refs[-3], refs[-2], refs[-1]
    capacity, table_rows = out_ref.shape[2], own_ref.shape[2]
    parts = capacity // LANES
    kind = pl.program_id(0)
    table = jnp.concatenate([own_ref[0], oth_ref[0]], axis=0)
    lane_ids = ids((LANES, LANES), 1)
    for block in range(blocks):
        rows = msg_refs[block][request_row:, :]
        lines = rows.shape[0]
        pieces = lines // parts
        here = rows[:parts]
        for k in range(1, pieces):
            here = jnp.where(kind == k, rows[k * parts : (k + 1) * parts], here)
        here = jnp.concatenate([here] * (8 // min(parts, 8)), axis=0).astype(jnp.float32)
        columns = jnp.transpose(here).astype(jnp.int32)
        hot = []
        for part in range(parts):
            column = columns[:, part : part + 1]
            low = jnp.broadcast_to((column & 127).astype(jnp.float32), (LANES, LANES))
            high = jnp.broadcast_to((column >> 7).astype(jnp.float32), (LANES, LANES))
            low, high = low.astype(jnp.bfloat16), high.astype(jnp.bfloat16)
            unit = one_zero(low == lane_ids)
            none = jnp.zeros_like(unit)
            hot.append(
                jnp.concatenate(
                    [
                        jnp.where(high == jnp.full((LANES, LANES), tile, jnp.bfloat16), unit, none)
                        for tile in range(table_rows // LANES)
                    ],
                    axis=1,
                )
            )
        out_ref[0, block] = dot(jnp.concatenate(hot, axis=0), table, NT).astype(jnp.bfloat16)


def relate_body(rels_here, kind, rels, blocks, edge_chunks, place_ref, *refs):
    msg_refs = refs[:blocks]
    pick_ref, own_ref, oth_ref, kept_ref, sent_ref, hold_ref = refs[blocks:]
    capacity = pick_ref.shape[2]
    half = capacity // 2
    first = place_ref[0] * capacity
    columns = own_ref.shape[2] // 2
    seed_row, degree_row, _, _ = message_rows(rels, edge_chunks, pick_ref.shape[0], capacity)

    def split(packed):
        slot = (packed >> SHIFT) - first
        mine = (slot >= 0) & (slot < capacity)
        upper = jnp.where(slot >= half, 1, 0)
        left = jnp.where(mine, slot - upper * half, -1).astype(jnp.float32)
        right = jnp.where(mine, (packed & LOW) + upper * SEEDS, -1).astype(jnp.float32)
        return jnp.transpose(left), right

    right_ids = ids((2 * SEEDS, LANES), 0)
    tiles = [(at, min(LANES, half - at)) for at in range(0, half, LANES)]
    left_ids = [ids((LANES, size), 1, at) for at, size in tiles]

    def counts(left, right, lines):
        left_hot, right_hot = [], []
        for line in lines:
            column = left[:, line : line + 1]
            pieces = []
            for (_, size), want in zip(tiles, left_ids):
                wide = jnp.broadcast_to(column, (LANES, size)).astype(jnp.bfloat16)
                pieces.append(one_zero(wide == want))
            left_hot.append(jnp.concatenate(pieces, axis=1))
            right_hot.append(one_zero(tiled(right[line : line + 1], 2 * SEEDS) == right_ids))
        table = dot(jnp.concatenate(right_hot, axis=1), jnp.concatenate(left_hot, axis=0))
        table = table.astype(jnp.bfloat16)
        return jnp.concatenate([table[:SEEDS], table[SEEDS:]], axis=1)

    for block in range(blocks):
        msg_ref = msg_refs[block]
        degree = msg_ref[degree_row : degree_row + rels, :].astype(jnp.float32)
        inverse = jnp.transpose(1.0 / jnp.maximum(degree, 1.0))
        spot = slice(block * SEEDS, (block + 1) * SEEDS)
        left, right = split(msg_ref[:seed_row, :])
        for order, rel in enumerate(rels_here):
            table = counts(left, right, [c * rels + rel for c in range(edge_chunks)])
            summed = dot(table, pick_ref[RELATION_SOURCE[rel], block])
            hold_ref[order, spot, :] = (summed * inverse[:, rel : rel + 1]).astype(jnp.bfloat16)
        left, right = split(msg_ref[seed_row : seed_row + 8, :])
        table = counts(left, right, [kind])
        hold_ref[len(rels_here), spot, :] = dot(table, pick_ref[kind, block]).astype(jnp.bfloat16)
    up = place_ref[2]
    for out_ref, piece in ((sent_ref, 1 - up), (kept_ref, up)):
        start = pl.multiple_of(piece * columns, columns)
        total = None
        for order, matrix in enumerate(tuple(rels_here) + (rels + kind,)):
            weight = jnp.concatenate(
                [own_ref[matrix, :, pl.ds(start, columns)], oth_ref[matrix, :, pl.ds(start, columns)]],
                axis=0,
            )
            term = dot(hold_ref[order], weight)
            total = term if total is None else total + term
        size, _, _, _, lanes = out_ref.shape
        for part in range(size):
            for block in range(blocks):
                for core in range(2):
                    at = (part * 2 + core) * lanes
                    out_ref[part, block, core] = total[
                        block * SEEDS : (block + 1) * SEEDS, at : at + lanes
                    ].astype(jnp.bfloat16)


def final_body(part_refs, out_ref):
    kinds = out_ref.shape[0]
    for kind in range(kinds):
        total = part_refs[4 * kind][...].astype(jnp.float32)
        for order in range(1, 4):
            total = total + part_refs[4 * kind + order][...].astype(jnp.float32)
        out_ref[kind] = jnp.transpose(jnp.maximum(total, 0.0)).astype(jnp.bfloat16)


def params(**more):
    return pltpu.CompilerParams(vmem_limit_bytes=VMEM_LIMIT, **more)


def per_device(groups, cores, features, weights, sample_owner, sample_row, edge_src, edge_dst, edge_count):
    kinds, width, table_rows = features.shape
    sampled = sample_row.shape[1]
    capacity = 2 * sampled // groups
    rels, edges = edge_src.shape
    full = weights.shape[2]
    blocks = groups // 2
    pieces_x = cores // 2
    devices = [(dp, mp) for dp in range(groups) for mp in range(cores)]

    def send(value, target):
        pairs = []
        for dp, mp in devices:
            to_dp, to_mp = target(dp, mp)
            pairs.append((dp * cores + mp, to_dp * cores + to_mp))
        return lax.ppermute(value, AXES, pairs)

    def swap_core(dp, mp):
        return dp, mp ^ 1

    def spread(step):
        def target(dp, mp):
            bit, core = (dp >> 1) & 1, mp & 1
            return ((dp ^ step) & ~2) | (core << 1), (mp & ~1) | bit

        return target

    dp, mp = lax.axis_index("dp"), lax.axis_index("mp")
    core, bit = mp & 1, (dp >> 1) & 1
    steps = [step for step in range(groups) if step & 2 == 0]

    features_oth = send(features, swap_core)
    weights_oth = send(weights, swap_core)

    edge_chunks = edges // LANES
    rows = message_rows(rels, edge_chunks, kinds, capacity)
    smem = pl.BlockSpec(memory_space=pltpu.SMEM)
    vmem = pl.BlockSpec(memory_space=pltpu.VMEM)
    message = jax.ShapeDtypeStruct((rows[3], LANES), jnp.int32)
    far = (mp >> 1) // (pieces_x // 2)
    place = jnp.stack([dp, core, far])
    packed = pl.pallas_call(
        functools.partial(prep_body, groups, capacity, steps),
        out_shape=[message] * blocks,
        in_specs=[smem] * 2 + [vmem] * 4,
        out_specs=[vmem] * blocks,
        scratch_shapes=[
            pltpu.VMEM((kinds, groups, capacity // LANES, LANES), jnp.int32),
            pltpu.VMEM((rows[3], LANES), jnp.int32),
        ],
        compiler_params=params(),
        name="prep",
    )(
        place,
        edge_count.reshape(1, rels),
        sample_owner.reshape(kinds, sampled // LANES, LANES),
        sample_row,
        edge_src,
        edge_dst,
    )
    listed = [send(value, spread(step)) for value, step in zip(packed, steps)]

    table_spec = pl.BlockSpec((1, width, table_rows), lambda t: (t, 0, 0))
    picked = pl.pallas_call(
        functools.partial(pick_body, blocks, rows[2]),
        out_shape=jax.ShapeDtypeStruct((kinds, blocks, capacity, 2 * width), jnp.bfloat16),
        grid=(kinds,),
        in_specs=[pl.BlockSpec((rows[3], LANES), lambda t: (0, 0))] * blocks + [table_spec] * 2,
        out_specs=pl.BlockSpec((1, blocks, capacity, 2 * width), lambda t: (t, 0, 0, 0)),
        compiler_params=params(),
        cost_estimate=pl.CostEstimate(
            flops=2 * kinds * blocks * capacity * table_rows * 2 * width,
            bytes_accessed=6 * 2**20,
            transcendentals=0,
        ),
        name="pick",
    )(*listed, features, features_oth)

    def merge(kept, got):
        return (kept.astype(jnp.float32) + got.astype(jnp.float32)).astype(jnp.bfloat16)

    halves = {}
    folded = {}
    for turn_kind, kind in enumerate(reversed(range(kinds))):
        rels_here = tuple(r for r in range(rels) if RELATION_TARGET[r] == kind)
        half_shape = jax.ShapeDtypeStruct(
            (pieces_x // 2, blocks, 2, SEEDS, full // cores), jnp.bfloat16
        )
        where = place
        if turn_kind >= 2:
            where, folded[kind + 2] = lax.optimization_barrier((place, folded[kind + 2]))
        kept, sent = pl.pallas_call(
            functools.partial(relate_body, rels_here, kind, rels, blocks, edge_chunks),
            out_shape=[half_shape] * 2,
            in_specs=[smem] + [vmem] * (blocks + 3),
            out_specs=[vmem] * 2,
            scratch_shapes=[
                pltpu.VMEM((len(rels_here) + 1, blocks * SEEDS, 2 * width), jnp.bfloat16)
            ],
            compiler_params=params(),
            cost_estimate=pl.CostEstimate(
                flops=2 * len(rels_here) * blocks * edges * capacity * SEEDS,
                bytes_accessed=6 * 2**20,
                transcendentals=0,
            ),
            name=f"relate{kind}",
        )(where, *listed, picked, weights, weights_oth)
        size = pieces_x // 2
        typed = merge(kept, send(sent, lambda d, m, size=size: (d, m ^ (2 * size))))
        while size > 1:
            size //= 2
            up = ((mp >> 1) // size) & 1
            pair = typed.reshape((2, size) + typed.shape[1:])
            kept = lax.dynamic_index_in_dim(pair, up, 0, keepdims=False)
            sent = lax.dynamic_index_in_dim(pair, 1 - up, 0, keepdims=False)
            typed = merge(kept, send(sent, lambda d, m, size=size: (d, m ^ (2 * size))))
        folded[kind] = typed[0]
    parts = []
    for kind in reversed(range(kinds)):
        typed = folded[kind]
        left = list(steps)
        for flip in [1] + [1 << i for i in range(3, groups.bit_length() - 1)]:
            keep = [i for i, step in enumerate(left) if step & flip == 0]
            away = [i for i, step in enumerate(left) if step & flip]
            kept = jnp.stack([typed[i] for i in keep])
            sent = jnp.stack([typed[i] for i in away])
            typed = merge(kept, send(sent, lambda d, m, flip=flip: (d ^ flip, m)))
            left = [left[i] for i in keep]
        mine = []
        for order, step in enumerate(left):
            for turn in range(2):
                value = lax.dynamic_index_in_dim(typed[order], bit ^ turn, 0, keepdims=False)

                def target(d, m, step=step, turn=turn):
                    return ((d ^ step) & ~2) | ((m & 1) << 1), (m & ~1) | (((d >> 1) & 1) ^ turn)

                mine.append(send(value, target))
        parts = mine + parts

    count = len(parts)
    return pl.pallas_call(
        lambda *refs: final_body(refs[:count], refs[count]),
        out_shape=jax.ShapeDtypeStruct((kinds, full // cores, SEEDS), jnp.bfloat16),
        in_specs=[vmem] * count,
        out_specs=vmem,
        compiler_params=params(),
        name="final",
    )(*parts)


def solution(mesh):
    return jax.shard_map(
        functools.partial(per_device, mesh.shape["dp"], mesh.shape["mp"]),
        mesh=mesh,
        in_specs=(
            P(None, "mp", "dp"),
            P(None, "mp", None),
            P(None, "dp", None),
            P(None, "dp"),
            P(None, "dp"),
            P(None, "dp"),
            P(None, "dp"),
        ),
        out_specs=P(None, "mp", "dp"),
        check_vma=False,
    )
```

```python
import functools

import jax
import jax.numpy as jnp
from jax import lax
from jax.experimental import pallas as pl
from jax.experimental.pallas import tpu as pltpu
from jax.sharding import PartitionSpec as P

SEEDS = 128
LANES = 128
SHIFT = 16
LOW = (1 << SHIFT) - 1

RELATION_SOURCE = (0, 1, 0, 1, 2, 0, 2, 1)
RELATION_TARGET = (1, 0, 0, 2, 1, 2, 0, 1)
AXES = ("dp", "mp")
NT = (((1,), (1,)), ((), ()))
NN = (((1,), (0,)), ((), ()))
VMEM_LIMIT = 24 * 1024 * 1024


def dot(left, right, dims=NN):
    return lax.dot_general(left, right, dims, preferred_element_type=jnp.float32)


def iota(shape, axis):
    return lax.broadcasted_iota(jnp.int32, shape, axis)


def as_bf16(mask):
    return jnp.where(mask, 1.0, 0.0).astype(jnp.bfloat16)


def tiled(row, lines):
    packed = jnp.broadcast_to(row, (16, LANES)).astype(jnp.bfloat16)
    return jnp.concatenate([packed] * (lines // 16), axis=0)


def one_zero(mask):
    one = jnp.ones(mask.shape, jnp.bfloat16)
    return jnp.where(mask, one, jnp.zeros_like(one))


def ids(shape, axis, start=0):
    return (iota(shape, axis) + start).astype(jnp.float32).astype(jnp.bfloat16)


def message_rows(rels, edge_chunks, kinds, capacity):
    seeds = rels * edge_chunks
    degrees = seeds + 8
    requests = degrees + 8
    return seeds, degrees, requests, requests + -(-kinds * capacity // LANES // 8) * 8


def prep_body(groups, capacity, steps, place_ref, count_ref, owner_ref, row_ref, src_ref, dst_ref, *refs):
    kinds, chunks, _ = owner_ref.shape
    out_refs, req_ref, hold_ref = refs[: len(steps)], refs[-2], refs[-1]
    rels, edges = src_ref.shape
    edge_chunks = edges // LANES
    seed_row, degree_row, request_row, _ = message_rows(rels, edge_chunks, kinds, capacity)
    parts = capacity // LANES
    stack = chunks * groups
    upper = as_bf16(iota((LANES, LANES), 0) <= iota((LANES, LANES), 1))
    ones = jnp.ones((LANES, LANES), jnp.bfloat16)
    line, other = iota((stack, stack), 0), iota((stack, stack), 1)
    earlier = as_bf16((other < line) & (line % groups == other % groups))
    owner_ids = iota((groups, LANES), 0)
    part_ids = iota((groups * parts, LANES), 0)
    lane_ids = ids((LANES, LANES), 0)
    tables = []
    for kind in range(kinds):
        owner = owner_ref[kind]
        row = jnp.concatenate(
            [row_ref[kind : kind + 1, c * LANES : (c + 1) * LANES] for c in range(chunks)], axis=0
        )
        hot = jnp.concatenate(
            [jnp.where(owner[c : c + 1] == owner_ids, 1.0, 0.0) for c in range(chunks)], axis=0
        )
        hot16 = hot.astype(jnp.bfloat16)
        totals = dot(hot16, ones).astype(jnp.bfloat16)
        inclusive = dot(hot16, upper) + dot(earlier, totals)
        ranks = jnp.sum((hot * inclusive).reshape(chunks, groups, LANES), axis=1)
        table = owner * capacity + ranks.astype(jnp.int32) - 1
        tables.append(table)
        part, low = table >> 7, (table & 127).astype(jnp.float32)
        high_digit, low_digit = (row >> 7).astype(jnp.float32), (row & 127).astype(jnp.float32)
        left = []
        for c in range(chunks):
            mask = part[c : c + 1] == part_ids
            left.append(
                jnp.concatenate(
                    [
                        jnp.where(mask, high_digit[c : c + 1], 0.0),
                        jnp.where(mask, low_digit[c : c + 1], 0.0),
                    ],
                    axis=0,
                )
            )
        left = jnp.concatenate(left, axis=1).astype(jnp.bfloat16)
        right = jnp.concatenate(
            [one_zero(tiled(low[c : c + 1], LANES) == lane_ids) for c in range(chunks)], axis=1
        )
        picked = dot(left, right, NT)
        rows = picked[: groups * parts] * 128.0 + picked[groups * parts :]
        rows = rows.astype(jnp.int32)
        for group in range(groups):
            req_ref[kind, group] = rows[group * parts : (group + 1) * parts]
    rel_ids = iota((rels, LANES), 0)
    wide = []
    for c in range(chunks):
        line = jnp.zeros((rels, LANES), jnp.int32)
        for kind in range(kinds):
            match = functools.reduce(
                lambda p, q: p | q, [rel_ids == r for r in range(rels) if RELATION_SOURCE[r] == kind]
            )
            line = jnp.where(match, tables[kind][c : c + 1], line)
        wide.append(line)
    limit = jnp.zeros((rels, LANES), jnp.int32)
    for rel in range(rels):
        limit = jnp.where(rel_ids == rel, count_ref[0, rel], limit)
    tallies = [jnp.zeros((SEEDS, LANES), jnp.bfloat16)] * rels
    target_ids = ids((SEEDS, LANES), 0)
    for e in range(edge_chunks):
        span = slice(e * LANES, (e + 1) * LANES)
        src, dst = src_ref[:, span], dst_ref[:, span]
        low, high = src & 127, src >> 7
        slot = jnp.zeros_like(src)
        for c in range(chunks):
            slot = jnp.where(high == c, jnp.take_along_axis(wide[c], low, axis=1), slot)
        live = iota((rels, LANES), 1) + e * LANES < limit
        hold_ref[e * rels : (e + 1) * rels, :] = jnp.where(live, (slot << SHIFT) | dst, -1)
        target = jnp.where(live, dst, -1).astype(jnp.float32)
        for rel in range(rels):
            tallies[rel] = tallies[rel] + one_zero(tiled(target[rel : rel + 1], SEEDS) == target_ids)
    eight = jnp.ones((8, LANES), jnp.bfloat16)
    degrees = [dot(eight, tally, NT)[:1] for tally in tallies]
    lane = iota((1, LANES), 1)
    seeds = [(table[:1] << SHIFT) | lane for table in tables]
    seeds = seeds + [jnp.full((1, LANES), -1, jnp.int32)] * (8 - kinds)
    hold_ref[seed_row : seed_row + 8, :] = jnp.concatenate(seeds, axis=0)
    hold_ref[degree_row : degree_row + rels, :] = jnp.concatenate(degrees, axis=0).astype(jnp.int32)
    for step, out_ref in zip(steps, out_refs):
        to = ((place_ref[0] ^ step) & ~2) | (place_ref[1] << 1)
        out_ref[:request_row, :] = hold_ref[:request_row, :]
        for kind in range(kinds):
            at = request_row + kind * parts
            out_ref[at : at + parts, :] = req_ref[kind, to]


def pick_body(blocks, request_row, *refs):
    msg_refs = refs[:blocks]
    own_ref, oth_ref, out_ref, table_ref, column_ref = refs[blocks:]
    kinds, _, capacity, width = out_ref.shape
    table_rows = own_ref.shape[2]
    parts = capacity // LANES
    lines = msg_refs[0].shape[0] - request_row
    lane_ids = ids((LANES, LANES), 1)
    for block in range(blocks):
        rows = msg_refs[block][request_row:, :].astype(jnp.float32)
        column_ref[block] = jnp.transpose(rows)

    def one_kind(kind, carry):
        table_ref[: width // 2, :] = own_ref[kind]
        table_ref[width // 2 :, :] = oth_ref[kind]

        def one_block(block, carry):
            columns = column_ref[block]
            hot = []
            for part in range(parts):
                column = columns[:, part : part + 1]
                for k in range(1, kinds):
                    other = columns[:, k * parts + part : k * parts + part + 1]
                    column = jnp.where(kind == k, other, column)
                column = column.astype(jnp.int32)
                low = jnp.broadcast_to((column & 127).astype(jnp.float32), (LANES, LANES))
                high = jnp.broadcast_to((column >> 7).astype(jnp.float32), (LANES, LANES))
                low, high = low.astype(jnp.bfloat16), high.astype(jnp.bfloat16)
                unit = one_zero(low == lane_ids)
                none = jnp.zeros_like(unit)
                hot.append(
                    jnp.concatenate(
                        [
                            jnp.where(high == jnp.full((LANES, LANES), tile, jnp.bfloat16), unit, none)
                            for tile in range(table_rows // LANES)
                        ],
                        axis=1,
                    )
                )
            hot = jnp.concatenate(hot, axis=0)
            out_ref[kind, block] = dot(hot, table_ref[...], NT).astype(jnp.bfloat16)
            return carry

        return lax.fori_loop(0, blocks, one_block, carry)

    lax.fori_loop(0, kinds, one_kind, 0)


def relate_body(rels_here, kind, rels, blocks, edge_chunks, place_ref, *refs):
    msg_refs = refs[:blocks]
    pick_ref, own_ref, oth_ref, kept_ref, sent_ref, hold_ref, note_ref = refs[blocks:]
    capacity = pick_ref.shape[2]
    half = capacity // 2
    first = place_ref[0] * capacity
    columns = own_ref.shape[2] // 2
    seed_row, degree_row, _, _ = message_rows(rels, edge_chunks, pick_ref.shape[0], capacity)

    def split(packed):
        slot = (packed >> SHIFT) - first
        mine = (slot >= 0) & (slot < capacity)
        upper = jnp.where(slot >= half, 1, 0)
        left = jnp.where(mine, slot - upper * half, -1).astype(jnp.float32)
        right = jnp.where(mine, (packed & LOW) + upper * SEEDS, -1).astype(jnp.float32)
        return jnp.transpose(left), right

    right_ids = ids((2 * SEEDS, LANES), 0)
    tiles = [(at, min(LANES, half - at)) for at in range(0, half, LANES)]
    left_ids = [ids((LANES, size), 1, at) for at, size in tiles]

    def counts(left, right, lines):
        left_hot, right_hot = [], []
        for line in lines:
            column = left[:, line : line + 1]
            pieces = []
            for (_, size), want in zip(tiles, left_ids):
                wide = jnp.broadcast_to(column, (LANES, size)).astype(jnp.bfloat16)
                pieces.append(one_zero(wide == want))
            left_hot.append(jnp.concatenate(pieces, axis=1))
            right_hot.append(one_zero(tiled(right[line : line + 1], 2 * SEEDS) == right_ids))
        table = dot(jnp.concatenate(right_hot, axis=1), jnp.concatenate(left_hot, axis=0))
        table = table.astype(jnp.bfloat16)
        return jnp.concatenate([table[:SEEDS], table[SEEDS:]], axis=1)

    for block in range(blocks):
        note_ref[block] = msg_refs[block][: note_ref.shape[1], :]

    def one_block(block, carry):
        degree = note_ref[block, degree_row : degree_row + rels, :].astype(jnp.float32)
        inverse = jnp.transpose(1.0 / jnp.maximum(degree, 1.0))
        spot = pl.ds(pl.multiple_of(block * SEEDS, SEEDS), SEEDS)
        left, right = split(note_ref[block, :seed_row, :])
        for order, rel in enumerate(rels_here):
            table = counts(left, right, [c * rels + rel for c in range(edge_chunks)])
            summed = dot(table, pick_ref[RELATION_SOURCE[rel], block])
            hold_ref[order, spot, :] = (summed * inverse[:, rel : rel + 1]).astype(jnp.bfloat16)
        left, right = split(note_ref[block, seed_row : seed_row + 8, :])
        table = counts(left, right, [kind])
        hold_ref[len(rels_here), spot, :] = dot(table, pick_ref[kind, block]).astype(jnp.bfloat16)
        return carry

    lax.fori_loop(0, blocks, one_block, 0)
    up = place_ref[2]
    for out_ref, piece in ((sent_ref, 1 - up), (kept_ref, up)):
        start = pl.multiple_of(piece * columns, columns)
        total = None
        for order, matrix in enumerate(tuple(rels_here) + (rels + kind,)):
            weight = jnp.concatenate(
                [own_ref[matrix, :, pl.ds(start, columns)], oth_ref[matrix, :, pl.ds(start, columns)]],
                axis=0,
            )
            term = dot(hold_ref[order], weight)
            total = term if total is None else total + term
        size, _, _, _, lanes = out_ref.shape
        for part in range(size):
            for block in range(blocks):
                for core in range(2):
                    at = (part * 2 + core) * lanes
                    out_ref[part, block, core] = total[
                        block * SEEDS : (block + 1) * SEEDS, at : at + lanes
                    ].astype(jnp.bfloat16)


def final_body(part_refs, out_ref):
    for kind in range(out_ref.shape[0]):
        total = part_refs[0][kind].astype(jnp.float32)
        for ref in part_refs[1:]:
            total = total + ref[kind].astype(jnp.float32)
        out_ref[kind] = jnp.transpose(jnp.maximum(total, 0.0)).astype(jnp.bfloat16)


def params(**more):
    return pltpu.CompilerParams(vmem_limit_bytes=VMEM_LIMIT, **more)


def per_device(groups, cores, features, weights, sample_owner, sample_row, edge_src, edge_dst, edge_count):
    kinds, width, table_rows = features.shape
    sampled = sample_row.shape[1]
    capacity = 2 * sampled // groups
    rels, edges = edge_src.shape
    full = weights.shape[2]
    blocks = groups // 2
    pieces_x = cores // 2
    devices = [(dp, mp) for dp in range(groups) for mp in range(cores)]

    def send(value, target):
        pairs = []
        for dp, mp in devices:
            to_dp, to_mp = target(dp, mp)
            pairs.append((dp * cores + mp, to_dp * cores + to_mp))
        return lax.ppermute(value, AXES, pairs)

    def swap_core(dp, mp):
        return dp, mp ^ 1

    def spread(step):
        def target(dp, mp):
            bit, core = (dp >> 1) & 1, mp & 1
            return ((dp ^ step) & ~2) | (core << 1), (mp & ~1) | bit

        return target

    dp, mp = lax.axis_index("dp"), lax.axis_index("mp")
    core, bit = mp & 1, (dp >> 1) & 1
    steps = [step for step in range(groups) if step & 2 == 0]

    features_oth = send(features, swap_core)
    weights_oth = send(weights, swap_core)

    edge_chunks = edges // LANES
    rows = message_rows(rels, edge_chunks, kinds, capacity)
    smem = pl.BlockSpec(memory_space=pltpu.SMEM)
    vmem = pl.BlockSpec(memory_space=pltpu.VMEM)
    message = jax.ShapeDtypeStruct((rows[3], LANES), jnp.int32)
    far = (mp >> 1) // (pieces_x // 2)
    place = jnp.stack([dp, core, far])
    packed = pl.pallas_call(
        functools.partial(prep_body, groups, capacity, steps),
        out_shape=[message] * blocks,
        in_specs=[smem] * 2 + [vmem] * 4,
        out_specs=[vmem] * blocks,
        scratch_shapes=[
            pltpu.VMEM((kinds, groups, capacity // LANES, LANES), jnp.int32),
            pltpu.VMEM((rows[3], LANES), jnp.int32),
        ],
        compiler_params=params(),
        name="prep",
    )(
        place,
        edge_count.reshape(1, rels),
        sample_owner.reshape(kinds, sampled // LANES, LANES),
        sample_row,
        edge_src,
        edge_dst,
    )
    listed = [send(value, spread(step)) for value, step in reversed(list(zip(packed, steps)))]
    listed = listed[::-1]

    picked = pl.pallas_call(
        functools.partial(pick_body, blocks, rows[2]),
        out_shape=jax.ShapeDtypeStruct((kinds, blocks, capacity, 2 * width), jnp.bfloat16),
        in_specs=[vmem] * (blocks + 2),
        out_specs=vmem,
        scratch_shapes=[
            pltpu.VMEM((2 * width, table_rows), jnp.bfloat16),
            pltpu.VMEM((blocks, LANES, rows[3] - rows[2]), jnp.float32),
        ],
        compiler_params=params(),
        cost_estimate=pl.CostEstimate(
            flops=2 * kinds * blocks * capacity * table_rows * 2 * width,
            bytes_accessed=6 * 2**20,
            transcendentals=0,
        ),
        name="pick",
    )(*listed, features, features_oth)

    def merge(kept, got):
        return (kept.astype(jnp.float32) + got.astype(jnp.float32)).astype(jnp.bfloat16)

    def fold_dp(typed):
        left = list(steps)
        for flip in [1] + [1 << i for i in range(3, groups.bit_length() - 1)]:
            keep = [i for i, step in enumerate(left) if step & flip == 0]
            away = [i for i, step in enumerate(left) if step & flip]
            kept = jnp.stack([typed[i] for i in keep])
            sent = jnp.stack([typed[i] for i in away])
            typed = merge(kept, send(sent, lambda d, m, flip=flip: (d ^ flip, m)))
            left = [left[i] for i in keep]
        return typed, left

    def fold_x(kept, got):
        size = pieces_x // 2
        typed = merge(kept, got)
        while size > 1:
            size //= 2
            up = ((mp >> 1) // size) & 1
            pair = typed.reshape((2, size) + typed.shape[1:])
            kept = lax.dynamic_index_in_dim(pair, up, 0, keepdims=False)
            sent = lax.dynamic_index_in_dim(pair, 1 - up, 0, keepdims=False)
            typed = merge(kept, send(sent, lambda d, m, size=size: (d, m ^ (2 * size))))
        return typed[0]

    half_shape = jax.ShapeDtypeStruct(
        (pieces_x // 2, blocks, 2, SEEDS, full // cores), jnp.bfloat16
    )

    def relate(kind, where):
        rels_here = tuple(r for r in range(rels) if RELATION_TARGET[r] == kind)
        return pl.pallas_call(
            functools.partial(relate_body, rels_here, kind, rels, blocks, edge_chunks),
            out_shape=[half_shape] * 2,
            in_specs=[smem] + [vmem] * (blocks + 3),
            out_specs=[vmem] * 2,
            scratch_shapes=[
                pltpu.VMEM((len(rels_here) + 1, blocks * SEEDS, 2 * width), jnp.bfloat16),
                pltpu.VMEM((blocks, rows[2], LANES), jnp.int32),
            ],
            compiler_params=params(),
            cost_estimate=pl.CostEstimate(
                flops=2 * len(rels_here) * blocks * edges * capacity * SEEDS,
                bytes_accessed=6 * 2**20,
                transcendentals=0,
            ),
            name=f"relate{kind}",
        )(where, *listed, picked, weights, weights_oth)

    def cross_x(sent):
        return send(sent, lambda d, m: (d, m ^ pieces_x))

    kept_c, sent_c = relate(2, place)
    got_c = cross_x(sent_c)
    kept_b, sent_b = relate(1, place)
    folded_c = fold_x(kept_c, got_c)
    got_b = cross_x(sent_b)
    where, folded_c = lax.optimization_barrier((place, folded_c))
    kept_a, sent_a = relate(0, where)
    kept_b, sent_a = lax.optimization_barrier((kept_b, sent_a))
    got_a = cross_x(sent_a)
    folded_b = fold_x(kept_b, got_b)
    last_c, left = fold_dp(folded_c)
    last_b, left = fold_dp(folded_b)
    last_a, left = fold_dp(fold_x(kept_a, got_a))
    last = jnp.stack([last_a, last_b, last_c])
    parts = []
    for order, step in enumerate(left):
        for turn in range(2):
            value = lax.dynamic_index_in_dim(last[:, order], bit ^ turn, 1, keepdims=False)

            def target(d, m, step=step, turn=turn):
                return ((d ^ step) & ~2) | ((m & 1) << 1), (m & ~1) | (((d >> 1) & 1) ^ turn)

            parts.append(send(value, target))

    count = len(parts)
    return pl.pallas_call(
        lambda *refs: final_body(refs[:count], refs[count]),
        out_shape=jax.ShapeDtypeStruct((kinds, full // cores, SEEDS), jnp.bfloat16),
        in_specs=[vmem] * count,
        out_specs=vmem,
        compiler_params=params(),
        name="final",
    )(*parts)


def solution(mesh):
    return jax.shard_map(
        functools.partial(per_device, mesh.shape["dp"], mesh.shape["mp"]),
        mesh=mesh,
        in_specs=(
            P(None, "mp", "dp"),
            P(None, "mp", None),
            P(None, "dp", None),
            P(None, "dp"),
            P(None, "dp"),
            P(None, "dp"),
            P(None, "dp"),
        ),
        out_specs=P(None, "mp", "dp"),
        check_vma=False,
    )
```

```python
import functools

import jax
import jax.numpy as jnp
from jax import lax
from jax.experimental import pallas as pl
from jax.experimental.pallas import tpu as pltpu
from jax.sharding import PartitionSpec as P

SEEDS = 128
LANES = 128
SHIFT = 16
LOW = (1 << SHIFT) - 1

RELATION_SOURCE = (0, 1, 0, 1, 2, 0, 2, 1)
RELATION_TARGET = (1, 0, 0, 2, 1, 2, 0, 1)
AXES = ("dp", "mp")
NT = (((1,), (1,)), ((), ()))
NN = (((1,), (0,)), ((), ()))
HOT = jnp.float8_e4m3fn
VMEM_LIMIT = 24 * 1024 * 1024


def dot(left, right, dims=NN):
    return lax.dot_general(left, right, dims, preferred_element_type=jnp.float32)


def iota(shape, axis):
    return lax.broadcasted_iota(jnp.int32, shape, axis)


def as_bf16(mask):
    return jnp.where(mask, 1.0, 0.0).astype(jnp.bfloat16)


def tiled(row, lines):
    packed = jnp.broadcast_to(row, (16, LANES)).astype(jnp.bfloat16)
    return jnp.concatenate([packed] * (lines // 16), axis=0)


def one_zero(mask):
    one = jnp.ones(mask.shape, jnp.bfloat16)
    return jnp.where(mask, one, jnp.zeros_like(one))


def ids(shape, axis, start=0):
    return (iota(shape, axis) + start).astype(jnp.float32).astype(jnp.bfloat16)


def message_rows(rels, edge_chunks, kinds, capacity):
    seeds = rels * edge_chunks
    degrees = seeds + 8
    requests = degrees + 8
    return seeds, degrees, requests, requests + -(-kinds * capacity // LANES // 8) * 8


def prep_body(groups, capacity, steps, kinds, rels, place_ref, list_ref, *refs):
    out_refs, req_ref, hold_ref = refs[: len(steps)], refs[-2], refs[-1]
    edges = list_ref.shape[1]
    chunks = edges // LANES
    src_ref, dst_ref = list_ref.at[:rels], list_ref.at[rels : 2 * rels]
    edge_chunks = edges // LANES
    seed_row, degree_row, request_row, _ = message_rows(rels, edge_chunks, kinds, capacity)
    parts = capacity // LANES
    stack = chunks * groups
    upper = as_bf16(iota((LANES, LANES), 0) <= iota((LANES, LANES), 1))
    ones = jnp.ones((LANES, LANES), jnp.bfloat16)
    line, other = iota((stack, stack), 0), iota((stack, stack), 1)
    earlier = as_bf16((other < line) & (line % groups == other % groups))
    owner_ids = iota((groups, LANES), 0)
    part_ids = iota((groups * parts, LANES), 0)
    lane_ids = ids((LANES, LANES), 0)
    tables = []
    for kind in range(kinds):
        owner, row = (
            jnp.concatenate(
                [list_ref[at : at + 1, c * LANES : (c + 1) * LANES] for c in range(chunks)], axis=0
            )
            for at in (2 * rels + kind, 2 * rels + kinds + kind)
        )
        hot = jnp.concatenate(
            [jnp.where(owner[c : c + 1] == owner_ids, 1.0, 0.0) for c in range(chunks)], axis=0
        )
        hot16 = hot.astype(jnp.bfloat16)
        totals = dot(hot16, ones).astype(jnp.bfloat16)
        inclusive = dot(hot16, upper) + dot(earlier, totals)
        ranks = jnp.sum((hot * inclusive).reshape(chunks, groups, LANES), axis=1)
        table = owner * capacity + ranks.astype(jnp.int32) - 1
        tables.append(table)
        part, low = table >> 7, (table & 127).astype(jnp.float32)
        high_digit, low_digit = (row >> 7).astype(jnp.float32), (row & 127).astype(jnp.float32)
        left = []
        for c in range(chunks):
            mask = part[c : c + 1] == part_ids
            left.append(
                jnp.concatenate(
                    [
                        jnp.where(mask, high_digit[c : c + 1], 0.0),
                        jnp.where(mask, low_digit[c : c + 1], 0.0),
                    ],
                    axis=0,
                )
            )
        left = jnp.concatenate(left, axis=1).astype(jnp.bfloat16)
        right = jnp.concatenate(
            [one_zero(tiled(low[c : c + 1], LANES) == lane_ids) for c in range(chunks)], axis=1
        )
        picked = dot(left, right, NT)
        rows = picked[: groups * parts] * 128.0 + picked[groups * parts :]
        rows = rows.astype(jnp.int32)
        for group in range(groups):
            req_ref[kind, group] = rows[group * parts : (group + 1) * parts]
    rel_ids = iota((rels, LANES), 0)
    wide = []
    for c in range(chunks):
        line = jnp.zeros((rels, LANES), jnp.int32)
        for kind in range(kinds):
            match = functools.reduce(
                lambda p, q: p | q, [rel_ids == r for r in range(rels) if RELATION_SOURCE[r] == kind]
            )
            line = jnp.where(match, tables[kind][c : c + 1], line)
        wide.append(line)
    limit = jnp.zeros((rels, LANES), jnp.int32)
    for rel in range(rels):
        limit = jnp.where(rel_ids == rel, place_ref[3 + rel], limit)
    tallies = [jnp.zeros((SEEDS, LANES), jnp.bfloat16)] * rels
    target_ids = ids((SEEDS, LANES), 0)
    for e in range(edge_chunks):
        span = slice(e * LANES, (e + 1) * LANES)
        src, dst = src_ref[:, span], dst_ref[:, span]
        low, high = src & 127, src >> 7
        slot = jnp.zeros_like(src)
        for c in range(chunks):
            slot = jnp.where(high == c, jnp.take_along_axis(wide[c], low, axis=1), slot)
        live = iota((rels, LANES), 1) + e * LANES < limit
        hold_ref[e * rels : (e + 1) * rels, :] = jnp.where(live, (slot << SHIFT) | dst, -1)
        target = jnp.where(live, dst, -1).astype(jnp.float32)
        for rel in range(rels):
            tallies[rel] = tallies[rel] + one_zero(tiled(target[rel : rel + 1], SEEDS) == target_ids)
    eight = jnp.ones((8, LANES), jnp.bfloat16)
    degrees = [dot(eight, tally, NT)[:1] for tally in tallies]
    lane = iota((1, LANES), 1)
    seeds = [(table[:1] << SHIFT) | lane for table in tables]
    seeds = seeds + [jnp.full((1, LANES), -1, jnp.int32)] * (8 - kinds)
    hold_ref[seed_row : seed_row + 8, :] = jnp.concatenate(seeds, axis=0)
    hold_ref[degree_row : degree_row + rels, :] = jnp.concatenate(degrees, axis=0).astype(jnp.int32)
    for step, out_ref in zip(steps, out_refs):
        to = ((place_ref[0] ^ step) & ~2) | (place_ref[1] << 1)
        out_ref[:request_row, :] = hold_ref[:request_row, :]
        for kind in range(kinds):
            at = request_row + kind * parts
            out_ref[at : at + parts, :] = req_ref[kind, to]


def pick_body(blocks, request_row, *refs):
    msg_refs = refs[:blocks]
    table_ref, out_ref, column_ref = refs[blocks:]
    kinds, _, capacity, width = out_ref.shape
    table_rows = table_ref.shape[2]
    parts = capacity // LANES
    lane_ids = ids((LANES, LANES), 1)
    for block in range(blocks):
        rows = msg_refs[block][request_row:, :].astype(jnp.float32)
        column_ref[block] = jnp.transpose(rows)

    def one_kind(kind, carry):
        for block in range(blocks):
            columns = column_ref[block]
            hot = []
            for part in range(parts):
                column = columns[:, part : part + 1]
                for k in range(1, kinds):
                    other = columns[:, k * parts + part : k * parts + part + 1]
                    column = jnp.where(kind == k, other, column)
                column = column.astype(jnp.int32)
                low = jnp.broadcast_to((column & 127).astype(jnp.float32), (LANES, LANES))
                high = jnp.broadcast_to((column >> 7).astype(jnp.float32), (LANES, LANES))
                low, high = low.astype(jnp.bfloat16), high.astype(jnp.bfloat16)
                unit = one_zero(low == lane_ids)
                none = jnp.zeros_like(unit)
                hot.append(
                    jnp.concatenate(
                        [
                            jnp.where(high == jnp.full((LANES, LANES), tile, jnp.bfloat16), unit, none)
                            for tile in range(table_rows // LANES)
                        ],
                        axis=1,
                    )
                )
            hot = jnp.concatenate(hot, axis=0)
            out_ref[kind, block] = dot(hot, table_ref[kind], NT).astype(jnp.bfloat16)
        return carry

    lax.fori_loop(0, kinds, one_kind, 0)


def relate_body(rels_here, kind, rels, blocks, edge_chunks, place_ref, *refs):
    msg_refs = refs[:blocks]
    pick_ref, own_ref, oth_ref, kept_ref, sent_ref, hold_ref, note_ref = refs[blocks:]
    capacity = pick_ref.shape[2]
    half = capacity // 2
    first = place_ref[0] * capacity
    columns = own_ref.shape[2] // 2
    seed_row, degree_row, _, _ = message_rows(rels, edge_chunks, pick_ref.shape[0], capacity)

    def split(packed):
        slot = (packed >> SHIFT) - first
        mine = (slot >= 0) & (slot < capacity)
        upper = jnp.where(slot >= half, 1, 0)
        left = jnp.where(mine, slot - upper * half, -1).astype(jnp.float32)
        right = jnp.where(mine, (packed & LOW) + upper * SEEDS, -1).astype(jnp.float32)
        return left, right

    right_ids = ids((2 * SEEDS, LANES), 0)
    left_ids = ids((half, LANES), 0)

    def counts(left, right, lines):
        left_hot, right_hot = [], []
        for line in lines:
            left_hot.append(one_zero(tiled(left[line : line + 1], half) == left_ids).astype(HOT))
            right_hot.append(one_zero(tiled(right[line : line + 1], 2 * SEEDS) == right_ids).astype(HOT))
        table = dot(jnp.concatenate(right_hot, axis=1), jnp.concatenate(left_hot, axis=1), NT)
        table = table.astype(jnp.bfloat16)
        return jnp.concatenate([table[:SEEDS], table[SEEDS:]], axis=1)

    for block in range(blocks):
        note_ref[block] = msg_refs[block][: note_ref.shape[1], :]

    def one_block(block, carry):
        degree = note_ref[block, degree_row : degree_row + rels, :].astype(jnp.float32)
        inverse = jnp.transpose(1.0 / jnp.maximum(degree, 1.0))
        spot = pl.ds(pl.multiple_of(block * SEEDS, SEEDS), SEEDS)
        left, right = split(note_ref[block, :seed_row, :])
        for order, rel in enumerate(rels_here):
            table = counts(left, right, [c * rels + rel for c in range(edge_chunks)])
            summed = dot(table, pick_ref[RELATION_SOURCE[rel], block])
            hold_ref[order, spot, :] = (summed * inverse[:, rel : rel + 1]).astype(jnp.bfloat16)
        left, right = split(note_ref[block, seed_row : seed_row + 8, :])
        table = counts(left, right, [kind])
        hold_ref[len(rels_here), spot, :] = dot(table, pick_ref[kind, block]).astype(jnp.bfloat16)
        return carry

    lax.fori_loop(0, blocks, one_block, 0)
    up = place_ref[2]
    for out_ref, piece in ((sent_ref, 1 - up), (kept_ref, up)):
        start = pl.multiple_of(piece * columns, columns)
        total = None
        for order, matrix in enumerate(tuple(rels_here) + (rels + kind,)):
            weight = jnp.concatenate(
                [own_ref[matrix, :, pl.ds(start, columns)], oth_ref[matrix, :, pl.ds(start, columns)]],
                axis=0,
            )
            term = dot(hold_ref[order], weight)
            total = term if total is None else total + term
        size, _, _, _, lanes = out_ref.shape
        for part in range(size):
            for block in range(blocks):
                for core in range(2):
                    at = (part * 2 + core) * lanes
                    out_ref[part, block, core] = total[
                        block * SEEDS : (block + 1) * SEEDS, at : at + lanes
                    ].astype(jnp.bfloat16)


def final_body(part_refs, out_ref):
    each = len(part_refs) // 2
    at = 0
    for refs in (part_refs[:each], part_refs[each:]):
        for order in range(refs[0].shape[0]):
            total = refs[0][order].astype(jnp.float32)
            for ref in refs[1:]:
                total = total + ref[order].astype(jnp.float32)
            out_ref[at] = jnp.transpose(jnp.maximum(total, 0.0)).astype(jnp.bfloat16)
            at += 1


def params(**more):
    return pltpu.CompilerParams(vmem_limit_bytes=VMEM_LIMIT, **more)


def per_device(groups, cores, features, weights, sample_owner, sample_row, edge_src, edge_dst, edge_count):
    kinds, width, table_rows = features.shape
    sampled = sample_row.shape[1]
    capacity = 2 * sampled // groups
    rels, edges = edge_src.shape
    full = weights.shape[2]
    blocks = groups // 2
    pieces_x = cores // 2
    devices = [(dp, mp) for dp in range(groups) for mp in range(cores)]

    def send(value, target):
        pairs = []
        for dp, mp in devices:
            to_dp, to_mp = target(dp, mp)
            pairs.append((dp * cores + mp, to_dp * cores + to_mp))
        return lax.ppermute(value, AXES, pairs)

    def swap_core(dp, mp):
        return dp, mp ^ 1

    def spread(step):
        def target(dp, mp):
            bit, core = (dp >> 1) & 1, mp & 1
            return ((dp ^ step) & ~2) | (core << 1), (mp & ~1) | bit

        return target

    dp, mp = lax.axis_index("dp"), lax.axis_index("mp")
    core, bit = mp & 1, (dp >> 1) & 1
    steps = [step for step in range(groups) if step & 2 == 0]

    features_oth = send(features, swap_core)
    weights_oth = send(weights, swap_core)

    edge_chunks = edges // LANES
    rows = message_rows(rels, edge_chunks, kinds, capacity)
    smem = pl.BlockSpec(memory_space=pltpu.SMEM)
    vmem = pl.BlockSpec(memory_space=pltpu.VMEM)
    message = jax.ShapeDtypeStruct((rows[3], LANES), jnp.int32)
    far = (mp >> 1) // (pieces_x // 2)
    place = jnp.concatenate([jnp.stack([dp, core, far]), edge_count[:, 0]])
    lists = jnp.concatenate([edge_src, edge_dst, sample_owner[:, :, 0], sample_row])
    packed = pl.pallas_call(
        functools.partial(prep_body, groups, capacity, steps, kinds, rels),
        out_shape=[message] * blocks,
        in_specs=[smem, vmem],
        out_specs=[vmem] * blocks,
        scratch_shapes=[
            pltpu.VMEM((kinds, groups, capacity // LANES, LANES), jnp.int32),
            pltpu.VMEM((rows[3], LANES), jnp.int32),
        ],
        compiler_params=params(),
        name="prep",
    )(place, lists)
    listed = [send(value, spread(step)) for value, step in reversed(list(zip(packed, steps)))]
    listed = listed[::-1]

    picked = pl.pallas_call(
        functools.partial(pick_body, blocks, rows[2]),
        out_shape=jax.ShapeDtypeStruct((kinds, blocks, capacity, 2 * width), jnp.bfloat16),
        in_specs=[vmem] * (blocks + 1),
        out_specs=vmem,
        scratch_shapes=[
            pltpu.VMEM((blocks, LANES, rows[3] - rows[2]), jnp.float32),
        ],
        compiler_params=params(),
        cost_estimate=pl.CostEstimate(
            flops=2 * kinds * blocks * capacity * table_rows * 2 * width,
            bytes_accessed=6 * 2**20,
            transcendentals=0,
        ),
        name="pick",
    )(*listed, jnp.concatenate([features, features_oth], axis=1))

    def merge(kept, got):
        return (kept.astype(jnp.float32) + got.astype(jnp.float32)).astype(jnp.bfloat16)

    def fold_dp(typed):
        left = list(steps)
        for flip in [1] + [1 << i for i in range(3, groups.bit_length() - 1)]:
            keep = [i for i, step in enumerate(left) if step & flip == 0]
            away = [i for i, step in enumerate(left) if step & flip]
            kept = jnp.stack([typed[i] for i in keep])
            sent = jnp.stack([typed[i] for i in away])
            typed = merge(kept, send(sent, lambda d, m, flip=flip: (d ^ flip, m)))
            left = [left[i] for i in keep]
        return typed, left

    def fold_x(kept, got):
        size = pieces_x // 2
        typed = merge(kept, got)
        while size > 1:
            size //= 2
            up = ((mp >> 1) // size) & 1
            pair = typed.reshape((2, size) + typed.shape[1:])
            kept = lax.dynamic_index_in_dim(pair, up, 0, keepdims=False)
            sent = lax.dynamic_index_in_dim(pair, 1 - up, 0, keepdims=False)
            typed = merge(kept, send(sent, lambda d, m, size=size: (d, m ^ (2 * size))))
        return typed[0]

    half_shape = jax.ShapeDtypeStruct(
        (pieces_x // 2, blocks, 2, SEEDS, full // cores), jnp.bfloat16
    )

    def relate(kind, where):
        rels_here = tuple(r for r in range(rels) if RELATION_TARGET[r] == kind)
        return pl.pallas_call(
            functools.partial(relate_body, rels_here, kind, rels, blocks, edge_chunks),
            out_shape=[half_shape] * 2,
            in_specs=[smem] + [vmem] * (blocks + 3),
            out_specs=[vmem] * 2,
            scratch_shapes=[
                pltpu.VMEM((len(rels_here) + 1, blocks * SEEDS, 2 * width), jnp.bfloat16),
                pltpu.VMEM((blocks, rows[2], LANES), jnp.int32),
            ],
            compiler_params=params(),
            cost_estimate=pl.CostEstimate(
                flops=2 * len(rels_here) * blocks * edges * capacity * SEEDS,
                bytes_accessed=6 * 2**20,
                transcendentals=0,
            ),
            name=f"relate{kind}",
        )(where, *listed, picked, weights, weights_oth)

    def cross_x(sent):
        return send(sent, lambda d, m: (d, m ^ pieces_x))

    kept_c, sent_c = relate(2, place)
    got_c = cross_x(sent_c)
    kept_b, sent_b = relate(1, place)
    folded_c = fold_x(kept_c, got_c)
    got_b = cross_x(sent_b)
    where, folded_c = lax.optimization_barrier((place, folded_c))
    kept_a, sent_a = relate(0, where)
    kept_b, sent_a = lax.optimization_barrier((kept_b, sent_a))
    got_a = cross_x(sent_a)
    folded_b = fold_x(kept_b, got_b)
    def to_block(values):
        folds = [fold_dp(value) for value in values]
        last = jnp.stack([fold for fold, _ in folds])
        parts = []
        for order, step in enumerate(folds[0][1]):
            for turn in range(2):
                value = lax.dynamic_index_in_dim(last[:, order], bit ^ turn, 1, keepdims=False)

                def target(d, m, step=step, turn=turn):
                    return ((d ^ step) & ~2) | ((m & 1) << 1), (m & ~1) | (((d >> 1) & 1) ^ turn)

                parts.append(send(value, target))
        return parts

    parts = to_block([fold_x(kept_a, got_a)]) + to_block([folded_b, folded_c])

    count = len(parts)
    return pl.pallas_call(
        lambda *refs: final_body(refs[:count], refs[count]),
        out_shape=jax.ShapeDtypeStruct((kinds, full // cores, SEEDS), jnp.bfloat16),
        in_specs=[vmem] * count,
        out_specs=vmem,
        compiler_params=params(),
        name="final",
    )(*parts)


def solution(mesh):
    return jax.shard_map(
        functools.partial(per_device, mesh.shape["dp"], mesh.shape["mp"]),
        mesh=mesh,
        in_specs=(
            P(None, "mp", "dp"),
            P(None, "mp", None),
            P(None, "dp", None),
            P(None, "dp"),
            P(None, "dp"),
            P(None, "dp"),
            P(None, "dp"),
        ),
        out_specs=P(None, "mp", "dp"),
        check_vma=False,
    )
```

```python
import functools

import jax
import jax.numpy as jnp
from jax import lax
from jax.experimental import pallas as pl
from jax.experimental.pallas import tpu as pltpu
from jax.sharding import PartitionSpec as P

SEEDS = 128
LANES = 128
SHIFT = 16
LOW = (1 << SHIFT) - 1

RELATION_SOURCE = (0, 1, 0, 1, 2, 0, 2, 1)
RELATION_TARGET = (1, 0, 0, 2, 1, 2, 0, 1)
AXES = ("dp", "mp")
NT = (((1,), (1,)), ((), ()))
NN = (((1,), (0,)), ((), ()))
HOT = jnp.float8_e4m3fn
VMEM_LIMIT = 24 * 1024 * 1024
PREP_LIMIT = 62 * 1024 * 1024


def dot(left, right, dims=NN):
    return lax.dot_general(left, right, dims, preferred_element_type=jnp.float32)


def iota(shape, axis):
    return lax.broadcasted_iota(jnp.int32, shape, axis)


def as_bf16(mask):
    return jnp.where(mask, 1.0, 0.0).astype(jnp.bfloat16)


def tiled(row, lines):
    packed = jnp.broadcast_to(row, (16, LANES)).astype(jnp.bfloat16)
    return jnp.concatenate([packed] * (lines // 16), axis=0)


def one_zero(mask):
    one = jnp.ones(mask.shape, jnp.bfloat16)
    return jnp.where(mask, one, jnp.zeros_like(one))


def ids(shape, axis, start=0):
    return (iota(shape, axis) + start).astype(jnp.float32).astype(jnp.bfloat16)


def message_rows(rels, edge_chunks, kinds, capacity):
    seeds = rels * edge_chunks
    degrees = seeds + 8
    requests = degrees + 8
    return seeds, degrees, requests, requests + -(-kinds * capacity // LANES // 8) * 8


def prep_body(groups, capacity, steps, place_ref, *refs):
    sources, out_refs, refs = refs[:5], refs[5 : 5 + len(steps)], refs[5 + len(steps) :]
    req_ref, hold_ref, sems, targets = refs[0], refs[1], refs[2], refs[3:]
    loads = [
        pltpu.make_async_copy(source, target, sems.at[order])
        for order, (source, target) in enumerate(zip(sources, targets))
    ]
    for load in loads:
        load.start()
    for load in loads:
        load.wait()
    count_ref, owner_ref, row_ref, src_ref, dst_ref = targets
    kinds, chunks, _ = owner_ref.shape
    rels, edges = src_ref.shape
    edge_chunks = edges // LANES
    seed_row, degree_row, request_row, _ = message_rows(rels, edge_chunks, kinds, capacity)
    parts = capacity // LANES
    stack = chunks * groups
    upper = as_bf16(iota((LANES, LANES), 0) <= iota((LANES, LANES), 1))
    ones = jnp.ones((LANES, LANES), jnp.bfloat16)
    line, other = iota((stack, stack), 0), iota((stack, stack), 1)
    earlier = as_bf16((other < line) & (line % groups == other % groups))
    owner_ids = iota((groups, LANES), 0)
    part_ids = iota((groups * parts, LANES), 0)
    lane_ids = ids((LANES, LANES), 0)
    tables = []
    for kind in range(kinds):
        owner = owner_ref[kind]
        row = jnp.concatenate(
            [row_ref[kind : kind + 1, c * LANES : (c + 1) * LANES] for c in range(chunks)], axis=0
        )
        hot = jnp.concatenate(
            [jnp.where(owner[c : c + 1] == owner_ids, 1.0, 0.0) for c in range(chunks)], axis=0
        )
        hot16 = hot.astype(jnp.bfloat16)
        totals = dot(hot16, ones).astype(jnp.bfloat16)
        inclusive = dot(hot16, upper) + dot(earlier, totals)
        ranks = jnp.sum((hot * inclusive).reshape(chunks, groups, LANES), axis=1)
        table = owner * capacity + ranks.astype(jnp.int32) - 1
        tables.append(table)
        part, low = table >> 7, (table & 127).astype(jnp.float32)
        high_digit, low_digit = (row >> 7).astype(jnp.float32), (row & 127).astype(jnp.float32)
        left = []
        for c in range(chunks):
            mask = part[c : c + 1] == part_ids
            left.append(
                jnp.concatenate(
                    [
                        jnp.where(mask, high_digit[c : c + 1], 0.0),
                        jnp.where(mask, low_digit[c : c + 1], 0.0),
                    ],
                    axis=0,
                )
            )
        left = jnp.concatenate(left, axis=1).astype(jnp.bfloat16)
        right = jnp.concatenate(
            [one_zero(tiled(low[c : c + 1], LANES) == lane_ids) for c in range(chunks)], axis=1
        )
        picked = dot(left, right, NT)
        rows = picked[: groups * parts] * 128.0 + picked[groups * parts :]
        rows = rows.astype(jnp.int32)
        for group in range(groups):
            req_ref[kind, group] = rows[group * parts : (group + 1) * parts]
    rel_ids = iota((rels, LANES), 0)
    wide = []
    for c in range(chunks):
        line = jnp.zeros((rels, LANES), jnp.int32)
        for kind in range(kinds):
            match = functools.reduce(
                lambda p, q: p | q, [rel_ids == r for r in range(rels) if RELATION_SOURCE[r] == kind]
            )
            line = jnp.where(match, tables[kind][c : c + 1], line)
        wide.append(line)
    limit = jnp.zeros((rels, LANES), jnp.int32)
    for rel in range(rels):
        limit = jnp.where(rel_ids == rel, count_ref[0, rel], limit)
    tallies = [jnp.zeros((SEEDS, LANES), jnp.bfloat16)] * rels
    target_ids = ids((SEEDS, LANES), 0)
    for e in range(edge_chunks):
        span = slice(e * LANES, (e + 1) * LANES)
        src, dst = src_ref[:, span], dst_ref[:, span]
        low, high = src & 127, src >> 7
        slot = jnp.zeros_like(src)
        for c in range(chunks):
            slot = jnp.where(high == c, jnp.take_along_axis(wide[c], low, axis=1), slot)
        live = iota((rels, LANES), 1) + e * LANES < limit
        hold_ref[e * rels : (e + 1) * rels, :] = jnp.where(live, (slot << SHIFT) | dst, -1)
        target = jnp.where(live, dst, -1).astype(jnp.float32)
        for rel in range(rels):
            tallies[rel] = tallies[rel] + one_zero(tiled(target[rel : rel + 1], SEEDS) == target_ids)
    eight = jnp.ones((8, LANES), jnp.bfloat16)
    degrees = [dot(eight, tally, NT)[:1] for tally in tallies]
    lane = iota((1, LANES), 1)
    seeds = [(table[:1] << SHIFT) | lane for table in tables]
    seeds = seeds + [jnp.full((1, LANES), -1, jnp.int32)] * (8 - kinds)
    hold_ref[seed_row : seed_row + 8, :] = jnp.concatenate(seeds, axis=0)
    hold_ref[degree_row : degree_row + rels, :] = jnp.concatenate(degrees, axis=0).astype(jnp.int32)
    for step, out_ref in zip(steps, out_refs):
        to = ((place_ref[0] ^ step) & ~2) | (place_ref[1] << 1)
        out_ref[:request_row, :] = hold_ref[:request_row, :]
        for kind in range(kinds):
            at = request_row + kind * parts
            out_ref[at : at + parts, :] = req_ref[kind, to]


def pick_body(blocks, request_row, *refs):
    msg_refs = refs[:blocks]
    table_ref, out_ref, column_ref = refs[blocks:]
    kinds, _, capacity, width = out_ref.shape
    table_rows = table_ref.shape[2]
    parts = capacity // LANES
    lane_ids = ids((LANES, LANES), 1)
    for block in range(blocks):
        rows = msg_refs[block][request_row:, :].astype(jnp.float32)
        column_ref[block] = jnp.transpose(rows)

    def one_kind(kind, carry):
        for block in range(blocks):
            columns = column_ref[block]
            hot = []
            for part in range(parts):
                column = columns[:, part : part + 1]
                for k in range(1, kinds):
                    other = columns[:, k * parts + part : k * parts + part + 1]
                    column = jnp.where(kind == k, other, column)
                column = column.astype(jnp.int32)
                low = jnp.broadcast_to((column & 127).astype(jnp.float32), (LANES, LANES))
                high = jnp.broadcast_to((column >> 7).astype(jnp.float32), (LANES, LANES))
                low, high = low.astype(jnp.bfloat16), high.astype(jnp.bfloat16)
                unit = one_zero(low == lane_ids)
                none = jnp.zeros_like(unit)
                hot.append(
                    jnp.concatenate(
                        [
                            jnp.where(high == jnp.full((LANES, LANES), tile, jnp.bfloat16), unit, none)
                            for tile in range(table_rows // LANES)
                        ],
                        axis=1,
                    )
                )
            hot = jnp.concatenate(hot, axis=0)
            out_ref[kind, block] = dot(hot, table_ref[kind], NT).astype(jnp.bfloat16)
        return carry

    lax.fori_loop(0, kinds, one_kind, 0)


def relate_body(rels_here, kind, rels, blocks, edge_chunks, place_ref, *refs):
    msg_refs = refs[:blocks]
    pick_ref, own_ref, oth_ref, *out_refs, hold_ref, note_ref = refs[blocks:]
    capacity = pick_ref.shape[2]
    half = capacity // 2
    first = place_ref[0] * capacity
    columns = own_ref.shape[2] // 2
    seed_row, degree_row, _, _ = message_rows(rels, edge_chunks, pick_ref.shape[0], capacity)

    def split(packed):
        slot = (packed >> SHIFT) - first
        mine = (slot >= 0) & (slot < capacity)
        upper = jnp.where(slot >= half, 1, 0)
        left = jnp.where(mine, slot - upper * half, -1).astype(jnp.float32)
        right = jnp.where(mine, (packed & LOW) + upper * SEEDS, -1).astype(jnp.float32)
        return left, right

    right_ids = ids((2 * SEEDS, LANES), 0)
    left_ids = ids((half, LANES), 0)

    def counts(left, right, lines):
        left_hot, right_hot = [], []
        for line in lines:
            left_hot.append(one_zero(tiled(left[line : line + 1], half) == left_ids).astype(HOT))
            right_hot.append(one_zero(tiled(right[line : line + 1], 2 * SEEDS) == right_ids).astype(HOT))
        table = dot(jnp.concatenate(right_hot, axis=1), jnp.concatenate(left_hot, axis=1), NT)
        table = table.astype(jnp.bfloat16)
        return jnp.concatenate([table[:SEEDS], table[SEEDS:]], axis=1)

    for block in range(blocks):
        note_ref[block] = msg_refs[block][: note_ref.shape[1], :]

    def one_block(block, carry):
        degree = note_ref[block, degree_row : degree_row + rels, :].astype(jnp.float32)
        inverse = jnp.transpose(1.0 / jnp.maximum(degree, 1.0))
        spot = pl.ds(pl.multiple_of(block * SEEDS, SEEDS), SEEDS)
        left, right = split(note_ref[block, :seed_row, :])
        for order, rel in enumerate(rels_here):
            table = counts(left, right, [c * rels + rel for c in range(edge_chunks)])
            summed = dot(table, pick_ref[RELATION_SOURCE[rel], block])
            hold_ref[order, spot, :] = (summed * inverse[:, rel : rel + 1]).astype(jnp.bfloat16)
        left, right = split(note_ref[block, seed_row : seed_row + 8, :])
        table = counts(left, right, [kind])
        hold_ref[len(rels_here), spot, :] = dot(table, pick_ref[kind, block]).astype(jnp.bfloat16)
        return carry

    lax.fori_loop(0, blocks, one_block, 0)
    up = place_ref[2]
    for side in range(2):
        start = pl.multiple_of((up if side == 0 else 1 - up) * columns, columns)
        total = None
        for order, matrix in enumerate(tuple(rels_here) + (rels + kind,)):
            weight = jnp.concatenate(
                [own_ref[matrix, :, pl.ds(start, columns)], oth_ref[matrix, :, pl.ds(start, columns)]],
                axis=0,
            )
            term = dot(hold_ref[order], weight)
            total = term if total is None else total + term
        for turn in range(2):
            out_ref = out_refs[2 * side + turn]
            size, _, _, _, lanes = out_ref.shape
            for part in range(size):
                for order in range(blocks // 2):
                    block = 2 * order + turn
                    for core in range(2):
                        at = (part * 2 + core) * lanes
                        out_ref[part, order, core] = total[
                            block * SEEDS : (block + 1) * SEEDS, at : at + lanes
                        ].astype(jnp.bfloat16)


def final_body(part_refs, out_ref):
    each = len(part_refs) // 2
    at = 0
    for refs in (part_refs[:each], part_refs[each:]):
        for order in range(refs[0].shape[0]):
            total = refs[0][order].astype(jnp.float32)
            for ref in refs[1:]:
                total = total + ref[order].astype(jnp.float32)
            out_ref[at] = jnp.transpose(jnp.maximum(total, 0.0)).astype(jnp.bfloat16)
            at += 1


def params(**more):
    return pltpu.CompilerParams(vmem_limit_bytes=VMEM_LIMIT, **more)


def per_device(groups, cores, features, weights, sample_owner, sample_row, edge_src, edge_dst, edge_count):
    kinds, width, table_rows = features.shape
    sampled = sample_row.shape[1]
    capacity = 2 * sampled // groups
    rels, edges = edge_src.shape
    full = weights.shape[2]
    blocks = groups // 2
    pieces_x = cores // 2
    devices = [(dp, mp) for dp in range(groups) for mp in range(cores)]

    def send(value, target):
        pairs = []
        for dp, mp in devices:
            to_dp, to_mp = target(dp, mp)
            pairs.append((dp * cores + mp, to_dp * cores + to_mp))
        return lax.ppermute(value, AXES, pairs)

    def swap_core(dp, mp):
        return dp, mp ^ 1

    def spread(step):
        def target(dp, mp):
            bit, core = (dp >> 1) & 1, mp & 1
            return ((dp ^ step) & ~2) | (core << 1), (mp & ~1) | bit

        return target

    dp, mp = lax.axis_index("dp"), lax.axis_index("mp")
    core, bit = mp & 1, (dp >> 1) & 1
    steps = [step for step in range(groups) if step & 2 == 0]

    features_oth = send(features, swap_core)
    weights_oth = send(weights, swap_core)

    edge_chunks = edges // LANES
    rows = message_rows(rels, edge_chunks, kinds, capacity)
    smem = pl.BlockSpec(memory_space=pltpu.SMEM)
    vmem = pl.BlockSpec(memory_space=pltpu.VMEM)
    hbm = pl.BlockSpec(memory_space=pltpu.HBM)
    message = jax.ShapeDtypeStruct((rows[3], LANES), jnp.int32)
    far = (mp >> 1) // (pieces_x // 2)
    place = jnp.stack([dp, core, far])
    packed = pl.pallas_call(
        functools.partial(prep_body, groups, capacity, steps),
        out_shape=[message] * blocks,
        in_specs=[smem] + [hbm] * 5,
        out_specs=[vmem] * blocks,
        scratch_shapes=[
            pltpu.VMEM((kinds, groups, capacity // LANES, LANES), jnp.int32),
            pltpu.VMEM((rows[3], LANES), jnp.int32),
            pltpu.SemaphoreType.DMA((5,)),
            pltpu.SMEM((1, rels), jnp.int32),
            pltpu.VMEM((kinds, sampled // LANES, LANES), jnp.int32),
            pltpu.VMEM((kinds, sampled), jnp.int32),
            pltpu.VMEM((rels, edges), jnp.int32),
            pltpu.VMEM((rels, edges), jnp.int32),
        ],
        compiler_params=pltpu.CompilerParams(vmem_limit_bytes=PREP_LIMIT),
        name="prep",
    )(
        place,
        edge_count.reshape(1, rels),
        sample_owner.reshape(kinds, sampled // LANES, LANES),
        sample_row,
        edge_src,
        edge_dst,
    )
    listed = [send(value, spread(step)) for value, step in reversed(list(zip(packed, steps)))]
    listed = listed[::-1]

    picked = pl.pallas_call(
        functools.partial(pick_body, blocks, rows[2]),
        out_shape=jax.ShapeDtypeStruct((kinds, blocks, capacity, 2 * width), jnp.bfloat16),
        in_specs=[vmem] * (blocks + 1),
        out_specs=vmem,
        scratch_shapes=[
            pltpu.VMEM((blocks, LANES, rows[3] - rows[2]), jnp.float32),
        ],
        compiler_params=params(),
        cost_estimate=pl.CostEstimate(
            flops=2 * kinds * blocks * capacity * table_rows * 2 * width,
            bytes_accessed=6 * 2**20,
            transcendentals=0,
        ),
        name="pick",
    )(*listed, jnp.concatenate([features, features_oth], axis=1))

    def merge(*terms):
        total = terms[0].astype(jnp.float32)
        for term in terms[1:]:
            total = total + term.astype(jnp.float32)
        return total.astype(jnp.bfloat16)

    quadrant = jax.ShapeDtypeStruct(
        (pieces_x // 2, blocks // 2, 2, SEEDS, full // cores), jnp.bfloat16
    )

    def relate(kind, where):
        rels_here = tuple(r for r in range(rels) if RELATION_TARGET[r] == kind)
        return pl.pallas_call(
            functools.partial(relate_body, rels_here, kind, rels, blocks, edge_chunks),
            out_shape=[quadrant] * 4,
            in_specs=[smem] + [vmem] * (blocks + 3),
            out_specs=[vmem] * 4,
            scratch_shapes=[
                pltpu.VMEM((len(rels_here) + 1, blocks * SEEDS, 2 * width), jnp.bfloat16),
                pltpu.VMEM((blocks, rows[2], LANES), jnp.int32),
            ],
            compiler_params=params(),
            cost_estimate=pl.CostEstimate(
                flops=2 * len(rels_here) * blocks * edges * capacity * SEEDS,
                bytes_accessed=6 * 2**20,
                transcendentals=0,
            ),
            name=f"relate{kind}",
        )(where, *listed, picked, weights, weights_oth)

    def cross(quadrants):
        _, over_y, over_x, over_both = quadrants
        return (
            send(over_both, lambda d, m: (d ^ 1, m ^ pieces_x)),
            send(over_x, lambda d, m: (d, m ^ pieces_x)),
            send(over_y, lambda d, m: (d ^ 1, m)),
        )

    def fold(kept, got):
        typed = merge(kept, *got)
        size = pieces_x // 2
        while size > 1:
            size //= 2
            up = ((mp >> 1) // size) & 1
            pair = typed.reshape((2, size) + typed.shape[1:])
            kept = lax.dynamic_index_in_dim(pair, up, 0, keepdims=False)
            sent = lax.dynamic_index_in_dim(pair, 1 - up, 0, keepdims=False)
            typed = merge(kept, send(sent, lambda d, m, size=size: (d, m ^ (2 * size))))
        typed = typed[0]
        left = [step for step in steps if step & 1 == 0]
        for flip in [1 << i for i in range(3, groups.bit_length() - 1)]:
            keep = [i for i, step in enumerate(left) if step & flip == 0]
            away = [i for i, step in enumerate(left) if step & flip]
            kept = jnp.stack([typed[i] for i in keep])
            sent = jnp.stack([typed[i] for i in away])
            typed = merge(kept, send(sent, lambda d, m, flip=flip: (d ^ flip, m)))
            left = [left[i] for i in keep]
        return typed, left

    def to_block(folds):
        last = jnp.stack([typed for typed, _ in folds])
        parts = []
        for order, step in reversed(list(enumerate(folds[0][1]))):
            for turn in range(2):
                value = lax.dynamic_index_in_dim(last[:, order], bit ^ turn, 1, keepdims=False)

                def target(d, m, step=step, turn=turn):
                    return ((d ^ step) & ~2) | ((m & 1) << 1), (m & ~1) | (((d >> 1) & 1) ^ turn)

                parts.append(send(value, target))
        return parts

    quad_c = relate(2, place)
    got_c = cross(quad_c)
    quad_b = relate(1, place)
    fold_c = fold(quad_c[0], got_c)
    got_b = cross(quad_b)
    where, typed_c = lax.optimization_barrier((place, fold_c[0]))
    quad_a = relate(0, where)
    kept_b, *quad_a = lax.optimization_barrier((quad_b[0], *quad_a))
    got_a = cross(quad_a)
    fold_b = fold(kept_b, got_b)
    parts_bc = to_block([fold_b, (typed_c, fold_c[1])])
    kept_a, *parts_bc = lax.optimization_barrier((quad_a[0], *parts_bc))
    parts = to_block([fold(kept_a, got_a)]) + parts_bc

    count = len(parts)
    return pl.pallas_call(
        lambda *refs: final_body(refs[:count], refs[count]),
        out_shape=jax.ShapeDtypeStruct((kinds, full // cores, SEEDS), jnp.bfloat16),
        in_specs=[vmem] * count,
        out_specs=vmem,
        compiler_params=params(),
        name="final",
    )(*parts)


def solution(mesh):
    return jax.shard_map(
        functools.partial(per_device, mesh.shape["dp"], mesh.shape["mp"]),
        mesh=mesh,
        in_specs=(
            P(None, "mp", "dp"),
            P(None, "mp", None),
            P(None, "dp", None),
            P(None, "dp"),
            P(None, "dp"),
            P(None, "dp"),
            P(None, "dp"),
        ),
        out_specs=P(None, "mp", "dp"),
        check_vma=False,
    )
```
